128 devices in a mesh: pairs: 64 (over x, z, y), comp: 2 (over core).
Axes of the slice: x: 4, y: 4, z: 4, core: 2. Of those that a mesh axis runs over, the one named last changes fastest.
Arguments:
- effects: float32 [49, 524288], P(None, 'pairs'), may hold values from -24 to 24
- se_table: float32 [16, 49], replicated, may hold values from 0.5 to 2
- se_index: int32 [1024], P('pairs'), may hold values from 0 to 15
- base_root: float32 [16, 49, 49], replicated, may hold values from -0.875 to 0.875
- grid_scale: float32 [16], replicated, may hold values from 0.25 to 4
- comp_base: int32 [256], P('comp'), may hold values from 0 to 15
- comp_grid: int32 [256], P('comp'), may hold values from 0 to 15
- weights: float32 [256], P('comp'), may hold values from 0.2 to 5
Outputs:
- responsibility: float32 [256, 524288], P('comp', 'pairs')
- log_weights: float32 [256], P('comp')
- pair_loglik: float32 [524288], P('pairs')
The draws below stay inside these ranges and needn't reach their ends.
All inputs are finite; a program needn't handle non-finite values.
Results may differ from the reference program's by a relative error of at most 0.0003.
Values sent between devices are 32-bit elements; how exact they have to be, the bound alone decides.
A program may use at most 384 MiB of HBM per device.

```python
import math
import jax
import jax.numpy as jnp
from jax import lax

R = 49
NU = 16
NGRID = 16
NB = 16
TILE = 512
PAIRS = 524288
K = 256


def draw_effects(key, part):
    key_scale, key_base, key_flag, key_sign = jax.random.split(key, 4)
    values = 1.5 * jax.random.normal(key_base, (R, PAIRS), dtype=jnp.float32)
    return jnp.clip(values, -8.0, 8.0).astype(jnp.float32)


def plant(entries, rng, low, top_value):
    longest = entries.shape.index(max(entries.shape))
    spots = []
    for shift in (0, 1):
        where = [jax.random.randint(jax.random.fold_in(rng, axis), (), 0, length) for axis, length in enumerate(entries.shape)]
        where[longest] = (where[longest] + shift) % entries.shape[longest]
        spots.append(tuple(where))
    return entries.at[spots[0]].set(low).at[spots[1]].set(top_value)


def steps_of(stream_key, extent, pieces, least, top_value):
    gain, own = 1.0, jax.random.fold_in(stream_key, 6)
    for axis_at, blocks in pieces:
        heights = jnp.exp(jax.random.uniform(jax.random.fold_in(own, axis_at), (blocks,), jnp.float32, least / len(pieces), top_value / len(pieces)))
        gain = gain * jnp.repeat(heights, extent[axis_at] // blocks).reshape([-1 if axis == axis_at else 1 for axis in range(len(extent))])
    return gain


def normal_values(stream_key, shape, deviation, most, kind=jnp.bfloat16):
    return jnp.clip(deviation * jax.random.normal(stream_key, shape, jnp.float32), -most, most).astype(kind)


def setup_inputs(seed: int = 0) -> dict:
    arg_keys = jax.random.split(jax.random.key(seed), 9)
    return {
        "effects": draw_effects(jax.random.fold_in(arg_keys[8], 71), 0),
        "se_table": jnp.clip(jnp.exp(jax.random.uniform(arg_keys[1], (NB, R), jnp.float32, math.log(0.5), math.log(2.0))), 0.5, 2.0),
        "se_index": plant(jax.random.randint(arg_keys[2], (PAIRS // TILE,), 0, NB), jax.random.fold_in(arg_keys[2], 1), 0, NB - 1).astype(jnp.int32),
        "base_root": normal_values(arg_keys[3], (NU, R, R), R ** -0.5, 0.875, jnp.float32),
        "grid_scale": jnp.clip(jnp.exp(jax.random.uniform(arg_keys[4], (NGRID,), jnp.float32, math.log(0.25), math.log(4.0))), 0.25, 4.0),
        "comp_base": plant(jax.random.randint(arg_keys[5], (K,), 0, NU), jax.random.fold_in(arg_keys[5], 1), 0, NU - 1).astype(jnp.int32),
        "comp_grid": plant(jax.random.randint(arg_keys[6], (K,), 0, NGRID), jax.random.fold_in(arg_keys[6], 1), 0, NGRID - 1).astype(jnp.int32),
        "weights": jnp.clip(jnp.exp(math.log(5.0) - 3.218876 * jax.random.uniform(arg_keys[7], (K,), jnp.float32) ** steps_of(arg_keys[7], (K,), ((0, 2),), -0.2, 0.2)), 0.2, 5.0),
    }


def whiten_tables(se_table, base_root, grid_scale, comp_base, comp_grid):
    covariances = jnp.einsum('uij,ukj->uik', base_root, base_root, precision=lax.Precision.HIGHEST)
    picked = covariances[comp_base]
    scales = grid_scale[comp_grid]
    identity = jnp.eye(R, dtype=base_root.dtype)
    system = (scales * scales)[None, :, None, None] * picked[None]
    system = system + identity[None, None] * (se_table * se_table)[:, None, :, None]
    factor = jnp.linalg.cholesky(system)
    eye_full = jnp.broadcast_to(identity, factor.shape)
    inverse = jax.scipy.linalg.solve_triangular(factor, eye_full, lower=True)
    half_logdet = jnp.sum(jnp.log(jnp.diagonal(factor, axis1=2, axis2=3)), axis=-1)
    return (inverse, half_logdet)

def reference(effects, se_table, se_index, base_root, grid_scale, comp_base, comp_grid, weights):
    inverse, half_logdet = whiten_tables(se_table, base_root, grid_scale, comp_base, comp_grid)
    log_prior = jnp.log(weights)
    constant = 0.5 * R * math.log(2.0 * math.pi)
    tile_rows = effects.reshape(R, PAIRS // TILE, TILE).transpose(1, 0, 2)

    def one_tile(inputs):
        block_id, tile_data = inputs
        whitened = jnp.einsum('kij,jp->kip', inverse[block_id], tile_data, precision=lax.Precision.HIGHEST)
        quadratic = jnp.sum(whitened * whitened, axis=1)
        return log_prior[:, None] - 0.5 * quadratic - half_logdet[block_id][:, None] - constant
    scores = lax.map(one_tile, (se_index.astype(jnp.int32), tile_rows))
    scores = scores.transpose(1, 0, 2).reshape(K, PAIRS)
    score_max = jnp.max(scores, axis=0)
    score_sum = jnp.sum(jnp.exp(scores - score_max), axis=0)
    pair_loglik = score_max + jnp.log(score_sum)
    responsibility = jnp.exp(scores - pair_loglik)
    masses = jnp.sum(responsibility, axis=1)
    log_weights = jnp.log((masses + 1.0) / (PAIRS + K))
    return (responsibility, log_weights, pair_loglik)
```

```python
import math

import jax
import jax.numpy as jnp
from jax import lax
from jax.experimental import pallas as pl
from jax.experimental.pallas import tpu as pltpu
from jax.sharding import PartitionSpec as P

TILE = 512
R = 49
NBLK = 6
FEATS = 1280
OFF_BORDER = 960
OFF_LAST = 1008
OFF_DIAG = 1016
OFF_BIAS = 1256
HIGHEST = lax.Precision.HIGHEST


def row8(index):
    return pl.ds(pl.multiple_of(index * 8, 8), 8)


def invert_all(covar_ref, se2_ref, prior_ref, w_ref, d_ref, b_ref, c_ref, v_ref, x_ref):
    def w_at(g, f):
        return row8(g * FEATS + f)

    def d_at(g, block, a, c):
        return row8((g * NBLK + block) * 64 + a * 8 + c)

    def p_at(g, block, a, c):
        return row8((g * NBLK + block) * 64 + a * 8 + c)

    def pair_base(i, j):
        return (i * (i - 1) // 2 + j) * 64

    def cov(i, j):
        return jnp.broadcast_to(covar_ref[i, pl.ds(j, 1), :], (8, 128))

    def x_at(g, n):
        return row8(g * 72 + n)

    for g in range(2):
        se_last = se2_ref[48, g * 8 : g * 8 + 8, :]
        pivot = cov(48, 48) + se_last
        inv = 1.0 / pivot
        x_ref[x_at(g, 48), :] = jnp.log(pivot)
        w_ref[w_at(g, OFF_LAST), :] = -inv
        for i in range(48):
            edge = cov(48, i)
            x_ref[x_at(g, i), :] = edge
            w_ref[w_at(g, OFF_BORDER + i), :] = edge * inv

    def init_group(g, _):
        def init_row(i, _):
            edges = [x_ref[x_at(g, i * 8 + a), :] for a in range(8)]

            def init_pair(j, _):
                scaled = [w_ref[w_at(g, OFF_BORDER + j * 8 + c), :] for c in range(8)]
                base = pair_base(i, j)
                for a in range(8):
                    for c in range(8):
                        w_ref[w_at(g, base + a * 8 + c), :] = cov(i * 8 + a, j * 8 + c) - edges[a] * scaled[c]
                return 0

            lax.fori_loop(0, i, init_pair, 0)
            scaled = [w_ref[w_at(g, OFF_BORDER + i * 8 + c), :] for c in range(8)]
            for a in range(8):
                for c in range(a + 1):
                    entry = cov(i * 8 + a, i * 8 + c) - edges[a] * scaled[c]
                    if a == c:
                        entry = entry + se2_ref[i * 8 + a, pl.ds(pl.multiple_of(g * 8, 8), 8), :]
                    d_ref[d_at(g, i, a, c), :] = entry
            return 0

        lax.fori_loop(0, NBLK, init_row, 0)
        return 0

    lax.fori_loop(0, 2, init_group, 0)

    def pivot_block(k):
        for g in range(2):
            m = {(a, c): d_ref[d_at(g, k, a, c), :] for a in range(8) for c in range(a + 1)}
            product = None
            for s in range(8):
                p = m[s, s]
                product = p if product is None else product * p
                inv = 1.0 / p
                col = {a: (m[a, s] if a > s else m[s, a]) for a in range(8) if a != s}
                scaled = {a: col[a] * inv for a in col}
                for a in col:
                    for c in col:
                        if c <= a:
                            m[a, c] = m[a, c] - scaled[a] * col[c]
                for a in col:
                    m[max(a, s), min(a, s)] = scaled[a]
                m[s, s] = -inv
            x_ref[x_at(g, 48), :] = x_ref[x_at(g, 48), :] + jnp.log(product)
            for a in range(8):
                for c in range(8):
                    entry = m[max(a, c), min(a, c)]
                    if c <= a:
                        d_ref[d_at(g, k, a, c), :] = entry
                    v_ref[row8(g * 64 + a * 8 + c), :] = -entry

    def scale_block(g, k, j, swap):
        base = pair_base(k, j) if swap else pair_base(j, k)
        for half in range(2):
            rows = range(half * 4, half * 4 + 4)
            acc = {}
            for l in range(8):
                left = {}
                for a in rows:
                    left[a] = w_ref[w_at(g, base + (l * 8 + a if swap else a * 8 + l)), :]
                    c_ref[p_at(g, j, a, l), :] = left[a]
                for c in range(8):
                    right = v_ref[row8(g * 64 + l * 8 + c), :]
                    for a in rows:
                        term = left[a] * right
                        acc[a, c] = term if l == 0 else acc[a, c] + term
            for a in rows:
                for c in range(8):
                    b_ref[p_at(g, j, a, c), :] = acc[a, c]
        for a in range(8):
            for c in range(8):
                w_ref[w_at(g, base + (c * 8 + a if swap else a * 8 + c)), :] = b_ref[p_at(g, j, a, c), :]

    def scale_border(g, k):
        old = [w_ref[w_at(g, OFF_BORDER + k * 8 + m), :] for m in range(8)]
        total = w_ref[w_at(g, OFF_LAST), :]
        for c in range(8):
            new = old[0] * v_ref[row8(g * 64 + c), :]
            for l in range(1, 8):
                new = new + old[l] * v_ref[row8(g * 64 + l * 8 + c), :]
            x_ref[x_at(g, 49 + c), :] = new
            w_ref[w_at(g, OFF_BORDER + k * 8 + c), :] = new
            total = total - new * old[c]
        w_ref[w_at(g, OFF_LAST), :] = total

    def update_pair(g, i, j):
        base = pair_base(i, j)
        for half in range(2):
            rows = range(half * 4, half * 4 + 4)
            acc = {(a, c): w_ref[w_at(g, base + a * 8 + c), :] for a in rows for c in range(8)}
            for m in range(8):
                left = {a: b_ref[p_at(g, i, a, m), :] for a in rows}
                for c in range(8):
                    right = c_ref[p_at(g, j, c, m), :]
                    for a in rows:
                        acc[a, c] = acc[a, c] - left[a] * right
            for a in rows:
                for c in range(8):
                    w_ref[w_at(g, base + a * 8 + c), :] = acc[a, c]

    def update_diag(g, i):
        for rows in (range(0, 6), range(6, 8)):
            acc = {(a, c): d_ref[d_at(g, i, a, c), :] for a in rows for c in range(a + 1)}
            if rows[0]:
                edge = [w_ref[w_at(g, OFF_BORDER + i * 8 + c), :] for c in range(8)]
            for m in range(8):
                left = {a: b_ref[p_at(g, i, a, m), :] for a in rows}
                if rows[0]:
                    last = x_ref[x_at(g, 49 + m), :]
                for c in range(rows[-1] + 1):
                    right = c_ref[p_at(g, i, c, m), :]
                    for a in rows:
                        if c <= a:
                            acc[a, c] = acc[a, c] - left[a] * right
                    if rows[0]:
                        edge[c] = edge[c] - last * right
            for a, c in acc:
                d_ref[d_at(g, i, a, c), :] = acc[a, c]
            if rows[0]:
                for c in range(8):
                    w_ref[w_at(g, OFF_BORDER + i * 8 + c), :] = edge[c]

    def sweep(k, _):
        pivot_block(k)

        def scale_group(g, _):
            lax.fori_loop(0, k, lambda j, z: (scale_block(g, k, j, True), z)[1], 0)
            lax.fori_loop(k + 1, NBLK, lambda j, z: (scale_block(g, k, j, False), z)[1], 0)
            scale_border(g, k)
            return 0

        lax.fori_loop(0, 2, scale_group, 0)

        def update_group(g, _):
            def update_row(t, _):
                i = t + (t >= k).astype(jnp.int32)

                def update_one(s, _):
                    update_pair(g, i, s + (s >= k).astype(jnp.int32))
                    return 0

                lax.fori_loop(0, t, update_one, 0)
                update_diag(g, i)
                return 0

            lax.fori_loop(0, NBLK - 1, update_row, 0)
            return 0

        lax.fori_loop(0, 2, update_group, 0)
        return 0

    lax.fori_loop(0, NBLK, sweep, 0)

    zero = jnp.zeros((8, 128), jnp.float32)
    constant = 0.5 * R * math.log(2.0 * math.pi)

    def finish(g, _):
        w_ref[w_at(g, OFF_LAST), :] = 0.5 * w_ref[w_at(g, OFF_LAST), :]
        for n in range(1, 8):
            w_ref[w_at(g, OFF_LAST + n), :] = zero

        def finish_diag(i, _):
            for d in range(5):
                weight = 1.0 if 0 < d < 4 else 0.5
                for c in range(8):
                    a = (c + d) % 8
                    entry = d_ref[d_at(g, i, max(a, c), min(a, c)), :]
                    w_ref[w_at(g, OFF_DIAG + i * 40 + d * 8 + c), :] = weight * entry
            return 0

        lax.fori_loop(0, NBLK, finish_diag, 0)
        bias = jnp.broadcast_to(prior_ref[...], (8, 128)) - 0.5 * x_ref[x_at(g, 48), :] - constant
        coarse = bias.astype(jnp.bfloat16).astype(jnp.float32)
        w_ref[w_at(g, OFF_BIAS), :] = coarse
        w_ref[w_at(g, OFF_BIAS + 1), :] = bias - coarse
        for n in range(OFF_BIAS + 2, FEATS):
            w_ref[w_at(g, n), :] = zero
        return 0

    lax.fori_loop(0, 2, finish, 0)


def build_products(e_ref, hi_ref, lo_ref):
    width = e_ref.shape[1]
    blocks = [e_ref[i * 8 : i * 8 + 8, :] for i in range(NBLK)]

    def row(i):
        return jnp.broadcast_to(e_ref[i : i + 1, :], (8, width))

    groups = []
    for i in range(NBLK):
        for j in range(i):
            groups += [lambda i=i, j=j, a=a: row(i * 8 + a) * blocks[j] for a in range(8)]
    groups += [lambda j=j: row(48) * blocks[j] for j in range(NBLK)]
    groups += [lambda: row(48) * row(48)]
    for i in range(NBLK):
        for d in range(5):
            groups += [lambda i=i, d=d: blocks[i] * (pltpu.roll(blocks[i], 8 - d, 0) if d else blocks[i])]
    groups += [lambda: jnp.ones((8, width), jnp.float32)]
    groups += [lambda: jnp.zeros((8, width), jnp.float32)] * 2
    for n in range(0, len(groups), 2):
        both = jnp.concatenate([groups[n](), groups[n + 1]()], axis=0)
        head = both.astype(jnp.bfloat16)
        rest = (both - head.astype(jnp.float32)).astype(jnp.bfloat16)
        hi_ref[n * 8 : n * 8 + 16, :] = head
        lo_ref[n * 8 : n * 8 + 16, :] = rest


def score_kernel(
    e_ref, covar_ref, se2_ref, prior_ref, scores_ref, max_ref, sum_ref,
    w_ref, d_ref, b_ref, c_ref, v_ref, x_ref, hi_ref, lo_ref, left_ref,
):
    t = pl.program_id(0)

    @pl.when(t == 0)
    def _():
        invert_all(covar_ref, se2_ref, prior_ref, w_ref, d_ref, b_ref, c_ref, v_ref, x_ref)

    first = (t // 8) * (FEATS * 8) + t % 8
    for n in range(FEATS // 128):
        part = w_ref[pl.ds(first + n * 1024, 128, stride=8), :].T
        head = part.astype(jnp.bfloat16)
        left_ref[0:128, n * 128 : (n + 1) * 128] = head
        left_ref[128:256, n * 128 : (n + 1) * 128] = (part - head.astype(jnp.float32)).astype(jnp.bfloat16)
    build_products(e_ref, hi_ref, lo_ref)
    main = jnp.dot(left_ref[...], hi_ref[...], preferred_element_type=jnp.float32)
    rest = jnp.dot(left_ref[0:128, :], lo_ref[...], preferred_element_type=jnp.float32)
    scores = main[0:128] + (main[128:256] + rest)
    top = jnp.max(scores, axis=0, keepdims=True)
    scores_ref[...] = scores
    max_ref[0] = top
    sum_ref[0] = jnp.sum(jnp.exp(scores - top), axis=0, keepdims=True)


def finish_kernel(scores_ref, stats_ref, other_ref, resp_ref, loglik_ref, mass_ref):
    t = pl.program_id(0)
    m0, m1 = stats_ref[0:1, :], other_ref[0:1, :]
    top = jnp.maximum(m0, m1)
    total = stats_ref[1:2, :] * jnp.exp(m0 - top) + other_ref[1:2, :] * jnp.exp(m1 - top)
    loglik = top + jnp.log(total)
    loglik_ref[...] = loglik
    resp = jnp.exp(scores_ref[...] - loglik)
    resp_ref[...] = resp

    @pl.when(t == 0)
    def _():
        mass_ref[...] = jnp.zeros_like(mass_ref)

    part = resp[:, 0:128]
    for n in range(1, resp.shape[1] // 128):
        part = part + resp[:, n * 128 : (n + 1) * 128]
    mass_ref[...] = mass_ref[...] + part


def score_stage(effects, se_table, se_index, base_root, grid_scale, comp_base, comp_grid, weights):
    pairs = effects.shape[1]
    comps = comp_base.shape[0]
    tiles = pairs // TILE
    covariances = jnp.einsum("uij,ukj->iku", base_root, base_root, precision=HIGHEST)
    pick = (jnp.arange(base_root.shape[0], dtype=jnp.int32)[:, None] == comp_base[None]).astype(jnp.float32)
    scale = grid_scale[comp_grid]
    covar = jnp.einsum("iku,uc->ikc", covariances, pick, precision=HIGHEST) * (scale * scale)
    tile_se = se_table[se_index]
    se2 = jnp.broadcast_to((tile_se * tile_se).T[:, :, None], (R, tiles, comps))
    prior = jnp.log(weights)[None, :]

    whole = lambda shape: pl.BlockSpec(shape, lambda t: (0,) * len(shape))
    return pl.pallas_call(
        score_kernel,
        grid=(tiles,),
        in_specs=[
            pl.BlockSpec((R, TILE), lambda t: (0, t)),
            whole((R, R, comps)),
            whole((R, tiles, comps)),
            whole((1, comps)),
        ],
        out_specs=[
            pl.BlockSpec((comps, TILE), lambda t: (0, t)),
            pl.BlockSpec((1, 1, TILE), lambda t: (t, 0, 0)),
            pl.BlockSpec((1, 1, TILE), lambda t: (t, 0, 0)),
        ],
        out_shape=[
            jax.ShapeDtypeStruct((comps, pairs), jnp.float32),
            jax.ShapeDtypeStruct((tiles, 1, TILE), jnp.float32),
            jax.ShapeDtypeStruct((tiles, 1, TILE), jnp.float32),
        ],
        scratch_shapes=[
            pltpu.VMEM((2 * FEATS * 8, 128), jnp.float32),
            pltpu.VMEM((2 * NBLK * 64 * 8, 128), jnp.float32),
            pltpu.VMEM((2 * NBLK * 64 * 8, 128), jnp.float32),
            pltpu.VMEM((2 * NBLK * 64 * 8, 128), jnp.float32),
            pltpu.VMEM((2 * 64 * 8, 128), jnp.float32),
            pltpu.VMEM((2 * 72 * 8, 128), jnp.float32),
            pltpu.VMEM((FEATS, TILE), jnp.bfloat16),
            pltpu.VMEM((FEATS, TILE), jnp.bfloat16),
            pltpu.VMEM((256, FEATS), jnp.bfloat16),
        ],
        name="scores",
    )(effects, covar, se2, prior)


def per_device(effects, se_table, se_index, base_root, grid_scale, comp_base, comp_grid, weights):
    pairs = effects.shape[1]
    comps = comp_base.shape[0]
    scores, top, total = score_stage(
        effects, se_table, se_index, base_root, grid_scale, comp_base, comp_grid, weights
    )
    stats = jnp.stack([top.reshape(pairs), total.reshape(pairs)])
    other = lax.ppermute(stats, "comp", [(0, 1), (1, 0)])
    block = 2048
    resp, loglik, mass = pl.pallas_call(
        finish_kernel,
        grid=(pairs // block,),
        in_specs=[
            pl.BlockSpec((comps, block), lambda t: (0, t)),
            pl.BlockSpec((2, block), lambda t: (0, t)),
            pl.BlockSpec((2, block), lambda t: (0, t)),
        ],
        out_specs=[
            pl.BlockSpec((comps, block), lambda t: (0, t)),
            pl.BlockSpec((1, block), lambda t: (0, t)),
            pl.BlockSpec((comps, 128), lambda t: (0, 0)),
        ],
        out_shape=[
            jax.ShapeDtypeStruct((comps, pairs), jnp.float32),
            jax.ShapeDtypeStruct((1, pairs), jnp.float32),
            jax.ShapeDtypeStruct((comps, 128), jnp.float32),
        ],
        name="finish",
    )(scores, stats, other)
    local = jnp.sum(mass, axis=1)
    count = lax.axis_size("pairs")
    sent = lax.all_to_all(jnp.broadcast_to(local[None], (count, comps)), "pairs", 0, 0, tiled=True)
    masses = jnp.sum(sent, axis=0)
    log_weights = jnp.log((masses + 1.0) / (pairs * count + comps * lax.axis_size("comp")))
    return (resp, log_weights, loglik.reshape(pairs))


def solution(mesh):
    placed = (P(None, "pairs"), P(), P("pairs"), P(), P(), P("comp"), P("comp"), P("comp"))
    return jax.shard_map(
        per_device,
        mesh=mesh,
        in_specs=placed,
        out_specs=(P("comp", "pairs"), P("comp"), P("pairs")),
        check_vma=False,
    )
```

```python
import functools
import math

import jax
import jax.numpy as jnp
from jax import lax
from jax.experimental import pallas as pl
from jax.experimental.pallas import tpu as pltpu
from jax.sharding import PartitionSpec as P

TILE = 512
R = 49
NBLK = 6
FEATS = 1280
OFF_BORDER = 960
OFF_LAST = 1008
OFF_DIAG = 1016
OFF_BIAS = 1256
HIGHEST = lax.Precision.HIGHEST


def row8(index):
    return pl.ds(pl.multiple_of(index * 8, 8), 8)


def invert_all(covar_ref, se2_ref, weight_ref, w_ref, d_ref, b_ref, c_ref, v_ref, x_ref):
    def w_at(g, f):
        return row8(g * FEATS + f)

    def d_at(g, block, a, c):
        return row8((g * NBLK + block) * 64 + a * 8 + c)

    def p_at(g, block, a, c):
        return row8((g * NBLK + block) * 64 + a * 8 + c)

    def pair_base(i, j):
        return (i * (i - 1) // 2 + j) * 64

    def cov(i, j):
        return jnp.broadcast_to(covar_ref[i, pl.ds(j, 1), :], (8, 128))

    def x_at(g, n):
        return row8(g * 72 + n)

    for g in range(2):
        se_last = se2_ref[48, g * 8 : g * 8 + 8, :]
        pivot = cov(48, 48) + se_last
        inv = 1.0 / pivot
        x_ref[x_at(g, 48), :] = jnp.log(pivot)
        w_ref[w_at(g, OFF_LAST), :] = -inv
        for i in range(48):
            edge = cov(48, i)
            x_ref[x_at(g, i), :] = edge
            w_ref[w_at(g, OFF_BORDER + i), :] = edge * inv

    def init_group(g, _):
        def init_row(i, _):
            edges = [x_ref[x_at(g, i * 8 + a), :] for a in range(8)]

            def init_pair(j, _):
                scaled = [w_ref[w_at(g, OFF_BORDER + j * 8 + c), :] for c in range(8)]
                base = pair_base(i, j)
                for a in range(8):
                    for c in range(8):
                        w_ref[w_at(g, base + a * 8 + c), :] = cov(i * 8 + a, j * 8 + c) - edges[a] * scaled[c]
                return 0

            lax.fori_loop(0, i, init_pair, 0)
            scaled = [w_ref[w_at(g, OFF_BORDER + i * 8 + c), :] for c in range(8)]
            for a in range(8):
                for c in range(a + 1):
                    entry = cov(i * 8 + a, i * 8 + c) - edges[a] * scaled[c]
                    if a == c:
                        entry = entry + se2_ref[i * 8 + a, pl.ds(pl.multiple_of(g * 8, 8), 8), :]
                    d_ref[d_at(g, i, a, c), :] = entry
            return 0

        lax.fori_loop(0, NBLK, init_row, 0)
        return 0

    lax.fori_loop(0, 2, init_group, 0)

    def pivot_block(k):
        for g in range(2):
            m = {(a, c): d_ref[d_at(g, k, a, c), :] for a in range(8) for c in range(a + 1)}
            product = None
            for s in range(8):
                p = m[s, s]
                product = p if product is None else product * p
                inv = 1.0 / p
                col = {a: (m[a, s] if a > s else m[s, a]) for a in range(8) if a != s}
                scaled = {a: col[a] * inv for a in col}
                for a in col:
                    for c in col:
                        if c <= a:
                            m[a, c] = m[a, c] - scaled[a] * col[c]
                for a in col:
                    m[max(a, s), min(a, s)] = scaled[a]
                m[s, s] = -inv
            x_ref[x_at(g, 48), :] = x_ref[x_at(g, 48), :] + jnp.log(product)
            for a in range(8):
                for c in range(8):
                    entry = m[max(a, c), min(a, c)]
                    if c <= a:
                        d_ref[d_at(g, k, a, c), :] = entry
                    v_ref[row8(g * 64 + a * 8 + c), :] = -entry

    def scale_block(g, k, j, swap):
        base = pair_base(k, j) if swap else pair_base(j, k)
        for half in range(2):
            rows = range(half * 4, half * 4 + 4)
            acc = {}
            for l in range(8):
                left = {}
                for a in rows:
                    left[a] = w_ref[w_at(g, base + (l * 8 + a if swap else a * 8 + l)), :]
                    c_ref[p_at(g, j, a, l), :] = left[a]
                for c in range(8):
                    right = v_ref[row8(g * 64 + l * 8 + c), :]
                    for a in rows:
                        term = left[a] * right
                        acc[a, c] = term if l == 0 else acc[a, c] + term
            for a in rows:
                for c in range(8):
                    b_ref[p_at(g, j, a, c), :] = acc[a, c]
        for a in range(8):
            for c in range(8):
                w_ref[w_at(g, base + (c * 8 + a if swap else a * 8 + c)), :] = b_ref[p_at(g, j, a, c), :]

    def scale_border(g, k):
        old = [w_ref[w_at(g, OFF_BORDER + k * 8 + m), :] for m in range(8)]
        total = w_ref[w_at(g, OFF_LAST), :]
        for c in range(8):
            new = old[0] * v_ref[row8(g * 64 + c), :]
            for l in range(1, 8):
                new = new + old[l] * v_ref[row8(g * 64 + l * 8 + c), :]
            x_ref[x_at(g, 49 + c), :] = new
            w_ref[w_at(g, OFF_BORDER + k * 8 + c), :] = new
            total = total - new * old[c]
        w_ref[w_at(g, OFF_LAST), :] = total

    def update_pair(g, i, j):
        base = pair_base(i, j)
        for half in range(2):
            rows = range(half * 4, half * 4 + 4)
            acc = {(a, c): w_ref[w_at(g, base + a * 8 + c), :] for a in rows for c in range(8)}
            for m in range(8):
                left = {a: b_ref[p_at(g, i, a, m), :] for a in rows}
                for c in range(8):
                    right = c_ref[p_at(g, j, c, m), :]
                    for a in rows:
                        acc[a, c] = acc[a, c] - left[a] * right
            for a in rows:
                for c in range(8):
                    w_ref[w_at(g, base + a * 8 + c), :] = acc[a, c]

    def update_diag(g, i):
        for rows in (range(0, 6), range(6, 8)):
            acc = {(a, c): d_ref[d_at(g, i, a, c), :] for a in rows for c in range(a + 1)}
            if rows[0]:
                edge = [w_ref[w_at(g, OFF_BORDER + i * 8 + c), :] for c in range(8)]
            for m in range(8):
                left = {a: b_ref[p_at(g, i, a, m), :] for a in rows}
                if rows[0]:
                    last = x_ref[x_at(g, 49 + m), :]
                for c in range(rows[-1] + 1):
                    right = c_ref[p_at(g, i, c, m), :]
                    for a in rows:
                        if c <= a:
                            acc[a, c] = acc[a, c] - left[a] * right
                    if rows[0]:
                        edge[c] = edge[c] - last * right
            for a, c in acc:
                d_ref[d_at(g, i, a, c), :] = acc[a, c]
            if rows[0]:
                for c in range(8):
                    w_ref[w_at(g, OFF_BORDER + i * 8 + c), :] = edge[c]

    def sweep(k, _):
        pivot_block(k)

        def scale_group(g, _):
            lax.fori_loop(0, k, lambda j, z: (scale_block(g, k, j, True), z)[1], 0)
            lax.fori_loop(k + 1, NBLK, lambda j, z: (scale_block(g, k, j, False), z)[1], 0)
            scale_border(g, k)
            return 0

        lax.fori_loop(0, 2, scale_group, 0)

        def update_group(g, _):
            def update_row(t, _):
                i = t + (t >= k).astype(jnp.int32)

                def update_one(s, _):
                    update_pair(g, i, s + (s >= k).astype(jnp.int32))
                    return 0

                lax.fori_loop(0, t, update_one, 0)
                update_diag(g, i)
                return 0

            lax.fori_loop(0, NBLK - 1, update_row, 0)
            return 0

        lax.fori_loop(0, 2, update_group, 0)
        return 0

    lax.fori_loop(0, NBLK, sweep, 0)

    zero = jnp.zeros((8, 128), jnp.float32)
    constant = 0.5 * R * math.log(2.0 * math.pi)

    def finish(g, _):
        w_ref[w_at(g, OFF_LAST), :] = 0.5 * w_ref[w_at(g, OFF_LAST), :]
        for n in range(1, 8):
            w_ref[w_at(g, OFF_LAST + n), :] = zero

        def finish_diag(i, _):
            for d in range(5):
                weight = 1.0 if 0 < d < 4 else 0.5
                for c in range(8):
                    a = (c + d) % 8
                    entry = d_ref[d_at(g, i, max(a, c), min(a, c)), :]
                    w_ref[w_at(g, OFF_DIAG + i * 40 + d * 8 + c), :] = weight * entry
            return 0

        lax.fori_loop(0, NBLK, finish_diag, 0)
        bias = jnp.broadcast_to(jnp.log(weight_ref[...]), (8, 128)) - 0.5 * x_ref[x_at(g, 48), :] - constant
        coarse = bias.astype(jnp.bfloat16).astype(jnp.float32)
        w_ref[w_at(g, OFF_BIAS), :] = coarse
        w_ref[w_at(g, OFF_BIAS + 1), :] = bias - coarse
        for n in range(OFF_BIAS + 2, FEATS):
            w_ref[w_at(g, n), :] = zero
        return 0

    lax.fori_loop(0, 2, finish, 0)


def build_products(e_ref, hi_ref, lo_ref):
    width = e_ref.shape[1]
    blocks = [e_ref[i * 8 : i * 8 + 8, :] for i in range(NBLK)]

    def row(i):
        return jnp.broadcast_to(e_ref[i : i + 1, :], (8, width))

    groups = []
    for i in range(NBLK):
        for j in range(i):
            groups += [lambda i=i, j=j, a=a: row(i * 8 + a) * blocks[j] for a in range(8)]
    groups += [lambda j=j: row(48) * blocks[j] for j in range(NBLK)]
    groups += [lambda: row(48) * row(48)]
    for i in range(NBLK):
        for d in range(5):
            groups += [lambda i=i, d=d: blocks[i] * (pltpu.roll(blocks[i], 8 - d, 0) if d else blocks[i])]
    groups += [lambda: jnp.ones((8, width), jnp.float32)]
    groups += [lambda: jnp.zeros((8, width), jnp.float32)] * 2
    for n in range(0, len(groups), 2):
        both = jnp.concatenate([groups[n](), groups[n + 1]()], axis=0)
        head = both.astype(jnp.bfloat16)
        rest = (both - head.astype(jnp.float32)).astype(jnp.bfloat16)
        hi_ref[n * 8 : n * 8 + 16, :] = head
        lo_ref[n * 8 : n * 8 + 16, :] = rest


def prepare(se_ref, index_ref, root_ref, grid_ref, base_ref, level_ref, covar_ref, se2_ref, cov_ref, rows_ref):
    units = root_ref.shape[0]
    for u in range(units):
        root = root_ref[u]
        cov_ref[u * 56 : u * 56 + R, 0:R] = lax.dot_general(
            root, root, (((1,), (1,)), ((), ())), precision=HIGHEST, preferred_element_type=jnp.float32
        )
    comps = base_ref.shape[1]
    pick = (lax.broadcasted_iota(jnp.int32, (units, comps), 0) == base_ref[...]).astype(jnp.bfloat16)
    scale = jnp.zeros((1, comps), jnp.float32)
    for n in range(grid_ref.shape[0]):
        scale = jnp.where(level_ref[...] == n, grid_ref[n], scale)
    scale2 = scale * scale

    def one_row(i, _):
        part = cov_ref[pl.ds(i, units, stride=56), :].T[0:56]
        total = None
        for _ in range(3):
            head = part.astype(jnp.bfloat16)
            term = jnp.dot(head, pick, preferred_element_type=jnp.float32)
            total = term if total is None else total + term
            part = part - head.astype(jnp.float32)
        covar_ref[i] = total * scale2
        return 0

    lax.fori_loop(0, R, one_row, 0, unroll=7)
    for t in range(index_ref.shape[0]):
        rows_ref[t : t + 1, 0:R] = se_ref[pl.ds(index_ref[t], 1), :]
    squares = rows_ref[...] * rows_ref[...]
    for i in range(R):
        se2_ref[i] = jnp.broadcast_to(squares[:, i : i + 1], se2_ref.shape[1:])


def score_kernel(
    e_ref, se_ref, index_ref, root_ref, grid_ref, base_ref, level_ref, weight_ref, scores_ref, stats_ref,
    covar_ref, se2_ref, cov_ref, rows_ref, w_ref, d_ref, b_ref, c_ref, v_ref, x_ref, hi_ref, lo_ref, left_ref,
):
    t = pl.program_id(0)

    @pl.when(t == 0)
    def _():
        prepare(se_ref, index_ref, root_ref, grid_ref, base_ref, level_ref, covar_ref, se2_ref, cov_ref, rows_ref)
        invert_all(covar_ref, se2_ref, weight_ref, w_ref, d_ref, b_ref, c_ref, v_ref, x_ref)

    first = (t // 8) * (FEATS * 8) + t % 8
    for n in range(FEATS // 128):
        part = w_ref[pl.ds(first + n * 1024, 128, stride=8), :].T
        head = part.astype(jnp.bfloat16)
        left_ref[0:128, n * 128 : (n + 1) * 128] = head
        left_ref[128:256, n * 128 : (n + 1) * 128] = (part - head.astype(jnp.float32)).astype(jnp.bfloat16)
    build_products(e_ref, hi_ref, lo_ref)
    main = jnp.dot(left_ref[...], hi_ref[...], preferred_element_type=jnp.float32)
    rest = jnp.dot(left_ref[0:128, :], lo_ref[...], preferred_element_type=jnp.float32)
    scores = main[0:128] + (main[128:256] + rest)
    top = jnp.max(scores, axis=0, keepdims=True)
    scores_ref[:, pl.ds(pl.multiple_of(t * TILE, TILE), TILE)] = scores
    stats_ref[0:1, :] = top
    stats_ref[1:2, :] = jnp.sum(jnp.exp(scores - top), axis=0, keepdims=True)


def tail_kernel(
    count, all_pairs, all_comps, scores_ref, stats_ref, resp_ref, loglik_ref, logw_ref,
    other_ref, mine_ref, slots_ref, pair_sems, send_sems, recv_sems,
):
    chip, core = lax.axis_index("pairs"), lax.axis_index("comp")
    mesh_id = pl.DeviceIdType.MESH
    barrier = pltpu.get_barrier_semaphore()
    pl.semaphore_signal(barrier, inc=1, device_id=(chip, 1 - core), device_id_type=mesh_id)

    def greet(d, _):
        pl.semaphore_signal(barrier, inc=1, device_id=((chip + d) % count, core), device_id_type=mesh_id)
        return 0

    lax.fori_loop(1, count, greet, 0)
    pl.semaphore_wait(barrier, count)
    swap = pltpu.make_async_remote_copy(
        src_ref=stats_ref, dst_ref=other_ref, send_sem=pair_sems.at[0], recv_sem=pair_sems.at[1],
        device_id=(chip, 1 - core), device_id_type=mesh_id,
    )
    swap.start()
    swap.wait()

    def one_part(n, mass):
        cols = pl.ds(pl.multiple_of(n * TILE, TILE), TILE)
        m0, m1 = stats_ref[0:1, cols], other_ref[0:1, cols]
        top = jnp.maximum(m0, m1)
        total = stats_ref[1:2, cols] * jnp.exp(m0 - top) + other_ref[1:2, cols] * jnp.exp(m1 - top)
        loglik = top + jnp.log(total)
        loglik_ref[0:1, cols] = loglik
        resp = jnp.exp(scores_ref[:, cols] - loglik)
        resp_ref[:, cols] = resp
        for j in range(TILE // 128):
            mass = mass + resp[:, j * 128 : (j + 1) * 128]
        return mass

    mass = lax.fori_loop(0, scores_ref.shape[1] // TILE, one_part, jnp.zeros((128, 128), jnp.float32))
    own = jnp.sum(mass.T, axis=0, keepdims=True)
    mine_ref[...] = own
    slots_ref[chip] = own

    def copy_to(peer, slot):
        return pltpu.make_async_remote_copy(
            src_ref=mine_ref, dst_ref=slots_ref.at[slot], send_sem=send_sems.at[peer], recv_sem=recv_sems.at[slot],
            device_id=(peer, core), device_id_type=mesh_id,
        )

    def send(d, _):
        copy_to((chip + d) % count, chip).start()
        return 0

    lax.fori_loop(1, count, send, 0)

    def receive(d, _):
        peer = (chip + d) % count
        copy_to(peer, peer).wait_recv()
        return 0

    lax.fori_loop(1, count, receive, 0)
    masses = slots_ref[0]
    for n in range(1, count):
        masses = masses + slots_ref[n]
    logw_ref[...] = jnp.log((masses + 1.0) / (all_pairs + all_comps))

    def sent(d, _):
        copy_to((chip + d) % count, chip).wait_send()
        return 0

    lax.fori_loop(1, count, sent, 0)


def score_stage(effects, se_table, se_index, base_root, grid_scale, comp_base, comp_grid, weights):
    pairs = effects.shape[1]
    comps = comp_base.shape[0]
    tiles = pairs // TILE
    vmem = pl.BlockSpec(memory_space=pltpu.VMEM)
    smem = pl.BlockSpec(memory_space=pltpu.SMEM)
    return pl.pallas_call(
        score_kernel,
        grid=(tiles,),
        in_specs=[pl.BlockSpec((R, TILE), lambda t: (0, t)), vmem, smem, vmem, smem, vmem, vmem, vmem],
        out_specs=[vmem, pl.BlockSpec((2, TILE), lambda t: (0, t))],
        out_shape=[
            pltpu.VMEM((comps, pairs), jnp.float32),
            jax.ShapeDtypeStruct((2, pairs), jnp.float32),
        ],
        scratch_shapes=[
            pltpu.VMEM((R, 56, comps), jnp.float32),
            pltpu.VMEM((R, tiles, comps), jnp.float32),
            pltpu.VMEM((base_root.shape[0] * 56, 128), jnp.float32),
            pltpu.VMEM((tiles, 128), jnp.float32),
            pltpu.VMEM((2 * FEATS * 8, 128), jnp.float32),
            pltpu.VMEM((2 * NBLK * 64 * 8, 128), jnp.float32),
            pltpu.VMEM((2 * NBLK * 64 * 8, 128), jnp.float32),
            pltpu.VMEM((2 * NBLK * 64 * 8, 128), jnp.float32),
            pltpu.VMEM((2 * 64 * 8, 128), jnp.float32),
            pltpu.VMEM((2 * 72 * 8, 128), jnp.float32),
            pltpu.VMEM((FEATS, TILE), jnp.bfloat16),
            pltpu.VMEM((FEATS, TILE), jnp.bfloat16),
            pltpu.VMEM((256, FEATS), jnp.bfloat16),
        ],
        compiler_params=pltpu.CompilerParams(vmem_limit_bytes=44 * 1024 * 1024),
        name="scores",
    )(
        effects, se_table, se_index, base_root, grid_scale,
        comp_base.reshape(1, comps), comp_grid.reshape(1, comps), weights.reshape(1, comps),
    )


def per_device(effects, se_table, se_index, base_root, grid_scale, comp_base, comp_grid, weights):
    pairs = effects.shape[1]
    comps = comp_base.shape[0]
    scores, stats = score_stage(
        effects, se_table, se_index, base_root, grid_scale, comp_base, comp_grid, weights
    )
    count = lax.axis_size("pairs")
    vmem = pl.BlockSpec(memory_space=pltpu.VMEM)
    resp, loglik, logw = pl.pallas_call(
        functools.partial(tail_kernel, count, pairs * count, comps * lax.axis_size("comp")),
        in_specs=[vmem, vmem],
        out_specs=[vmem, vmem, vmem],
        out_shape=[
            pltpu.VMEM((comps, pairs), jnp.float32),
            jax.ShapeDtypeStruct((1, pairs), jnp.float32),
            jax.ShapeDtypeStruct((1, comps), jnp.float32),
        ],
        scratch_shapes=[
            pltpu.VMEM((2, pairs), jnp.float32),
            pltpu.VMEM((1, comps), jnp.float32),
            pltpu.VMEM((count, 1, comps), jnp.float32),
            pltpu.SemaphoreType.DMA((2,)),
            pltpu.SemaphoreType.DMA((count,)),
            pltpu.SemaphoreType.DMA((count,)),
        ],
        compiler_params=pltpu.CompilerParams(
            collective_id=0, has_side_effects=True, vmem_limit_bytes=24 * 1024 * 1024
        ),
        name="tail",
    )(scores, stats)
    return (resp, logw.reshape(comps), loglik.reshape(pairs))


def solution(mesh):
    placed = (P(None, "pairs"), P(), P("pairs"), P(), P(), P("comp"), P("comp"), P("comp"))
    return jax.shard_map(
        per_device,
        mesh=mesh,
        in_specs=placed,
        out_specs=(P("comp", "pairs"), P("comp"), P("pairs")),
        check_vma=False,
    )
```

```python
import functools
import math

import jax
import jax.numpy as jnp
from jax import lax
from jax.experimental import pallas as pl
from jax.experimental.pallas import tpu as pltpu
from jax.sharding import PartitionSpec as P

TILE = 512
R = 49
NBLK = 6
FEATS = 1280
OFF_BORDER = 960
OFF_LAST = 1008
OFF_DIAG = 1016
OFF_BIAS = 1256
HIGHEST = lax.Precision.HIGHEST


def row8(index):
    return pl.ds(pl.multiple_of(index * 8, 8), 8)


def invert_all(covar_ref, se2_ref, weight_ref, w_ref, d_ref, b_ref, c_ref, v_ref, x_ref):
    def w_at(g, f):
        return row8(g * FEATS + f)

    def d_at(g, block, a, c):
        return row8((g * NBLK + block) * 64 + a * 8 + c)

    def p_at(g, block, a, c):
        return row8((g * NBLK + block) * 64 + a * 8 + c)

    def pair_base(i, j):
        return (i * (i - 1) // 2 + j) * 64

    def cov(i, j):
        return jnp.broadcast_to(covar_ref[i, pl.ds(j, 1), :], (8, 128))

    def x_at(g, n):
        return row8(g * 72 + n)

    for g in range(2):
        se_last = se2_ref[48, g * 8 : g * 8 + 8, :]
        pivot = cov(48, 48) + se_last
        inv = 1.0 / pivot
        x_ref[x_at(g, 48), :] = jnp.log(pivot)
        w_ref[w_at(g, OFF_LAST), :] = -inv
        for i in range(48):
            edge = cov(48, i)
            x_ref[x_at(g, i), :] = edge
            w_ref[w_at(g, OFF_BORDER + i), :] = edge * inv

    def init_group(g, _):
        def init_row(i, _):
            edges = [x_ref[x_at(g, i * 8 + a), :] for a in range(8)]

            def init_pair(j, _):
                scaled = [w_ref[w_at(g, OFF_BORDER + j * 8 + c), :] for c in range(8)]
                base = pair_base(i, j)
                for a in range(8):
                    for c in range(8):
                        w_ref[w_at(g, base + a * 8 + c), :] = cov(i * 8 + a, j * 8 + c) - edges[a] * scaled[c]
                return 0

            lax.fori_loop(0, i, init_pair, 0)
            scaled = [w_ref[w_at(g, OFF_BORDER + i * 8 + c), :] for c in range(8)]
            for a in range(8):
                for c in range(a + 1):
                    entry = cov(i * 8 + a, i * 8 + c) - edges[a] * scaled[c]
                    if a == c:
                        entry = entry + se2_ref[i * 8 + a, pl.ds(pl.multiple_of(g * 8, 8), 8), :]
                    d_ref[d_at(g, i, a, c), :] = entry
            return 0

        lax.fori_loop(0, NBLK, init_row, 0)
        return 0

    lax.fori_loop(0, 2, init_group, 0)

    def pivot_block(k):
        for g in range(2):
            m = {(a, c): d_ref[d_at(g, k, a, c), :] for a in range(8) for c in range(a + 1)}
            product = None
            for s in range(8):
                p = m[s, s]
                product = p if product is None else product * p
                inv = 1.0 / p
                col = {a: (m[a, s] if a > s else m[s, a]) for a in range(8) if a != s}
                scaled = {a: col[a] * inv for a in col}
                for a in col:
                    for c in col:
                        if c <= a:
                            m[a, c] = m[a, c] - scaled[a] * col[c]
                for a in col:
                    m[max(a, s), min(a, s)] = scaled[a]
                m[s, s] = -inv
            x_ref[x_at(g, 48), :] = x_ref[x_at(g, 48), :] + jnp.log(product)
            for a in range(8):
                for c in range(8):
                    entry = m[max(a, c), min(a, c)]
                    if c <= a:
                        d_ref[d_at(g, k, a, c), :] = entry
                    v_ref[row8(g * 64 + a * 8 + c), :] = -entry

    def scale_block(g, k, j, swap):
        base = pair_base(k, j) if swap else pair_base(j, k)
        for half in range(2):
            rows = range(half * 4, half * 4 + 4)
            acc = {}
            for l in range(8):
                left = {}
                for a in rows:
                    left[a] = w_ref[w_at(g, base + (l * 8 + a if swap else a * 8 + l)), :]
                    c_ref[p_at(g, j, a, l), :] = left[a]
                for c in range(8):
                    right = v_ref[row8(g * 64 + l * 8 + c), :]
                    for a in rows:
                        term = left[a] * right
                        acc[a, c] = term if l == 0 else acc[a, c] + term
            for a in rows:
                for c in range(8):
                    b_ref[p_at(g, j, a, c), :] = acc[a, c]
        for a in range(8):
            for c in range(8):
                w_ref[w_at(g, base + (c * 8 + a if swap else a * 8 + c)), :] = b_ref[p_at(g, j, a, c), :]

    def scale_border(g, k):
        old = [w_ref[w_at(g, OFF_BORDER + k * 8 + m), :] for m in range(8)]
        total = w_ref[w_at(g, OFF_LAST), :]
        for c in range(8):
            new = old[0] * v_ref[row8(g * 64 + c), :]
            for l in range(1, 8):
                new = new + old[l] * v_ref[row8(g * 64 + l * 8 + c), :]
            x_ref[x_at(g, 49 + c), :] = new
            w_ref[w_at(g, OFF_BORDER + k * 8 + c), :] = new
            total = total - new * old[c]
        w_ref[w_at(g, OFF_LAST), :] = total

    def update_pair(g, i, j):
        base = pair_base(i, j)
        for half in range(2):
            rows = range(half * 4, half * 4 + 4)
            acc = {(a, c): w_ref[w_at(g, base + a * 8 + c), :] for a in rows for c in range(8)}
            for m in range(8):
                left = {a: b_ref[p_at(g, i, a, m), :] for a in rows}
                for c in range(8):
                    right = c_ref[p_at(g, j, c, m), :]
                    for a in rows:
                        acc[a, c] = acc[a, c] - left[a] * right
            for a in rows:
                for c in range(8):
                    w_ref[w_at(g, base + a * 8 + c), :] = acc[a, c]

    def update_diag(g, i):
        for rows in (range(0, 6), range(6, 8)):
            acc = {(a, c): d_ref[d_at(g, i, a, c), :] for a in rows for c in range(a + 1)}
            if rows[0]:
                edge = [w_ref[w_at(g, OFF_BORDER + i * 8 + c), :] for c in range(8)]
            for m in range(8):
                left = {a: b_ref[p_at(g, i, a, m), :] for a in rows}
                if rows[0]:
                    last = x_ref[x_at(g, 49 + m), :]
                for c in range(rows[-1] + 1):
                    right = c_ref[p_at(g, i, c, m), :]
                    for a in rows:
                        if c <= a:
                            acc[a, c] = acc[a, c] - left[a] * right
                    if rows[0]:
                        edge[c] = edge[c] - last * right
            for a, c in acc:
                d_ref[d_at(g, i, a, c), :] = acc[a, c]
            if rows[0]:
                for c in range(8):
                    w_ref[w_at(g, OFF_BORDER + i * 8 + c), :] = edge[c]

    def sweep(k, _):
        pivot_block(k)

        def scale_group(g, _):
            lax.fori_loop(0, k, lambda j, z: (scale_block(g, k, j, True), z)[1], 0)
            lax.fori_loop(k + 1, NBLK, lambda j, z: (scale_block(g, k, j, False), z)[1], 0)
            scale_border(g, k)
            return 0

        lax.fori_loop(0, 2, scale_group, 0)

        def update_group(g, _):
            def update_row(t, _):
                i = t + (t >= k).astype(jnp.int32)

                def update_one(s, _):
                    update_pair(g, i, s + (s >= k).astype(jnp.int32))
                    return 0

                lax.fori_loop(0, t, update_one, 0)
                update_diag(g, i)
                return 0

            lax.fori_loop(0, NBLK - 1, update_row, 0)
            return 0

        lax.fori_loop(0, 2, update_group, 0)
        return 0

    lax.fori_loop(0, NBLK, sweep, 0)

    zero = jnp.zeros((8, 128), jnp.float32)
    constant = 0.5 * R * math.log(2.0 * math.pi)

    def finish(g, _):
        w_ref[w_at(g, OFF_LAST), :] = 0.5 * w_ref[w_at(g, OFF_LAST), :]
        for n in range(1, 8):
            w_ref[w_at(g, OFF_LAST + n), :] = zero

        def finish_diag(i, _):
            for d in range(5):
                weight = 1.0 if 0 < d < 4 else 0.5
                for c in range(8):
                    a = (c + d) % 8
                    entry = d_ref[d_at(g, i, max(a, c), min(a, c)), :]
                    w_ref[w_at(g, OFF_DIAG + i * 40 + d * 8 + c), :] = weight * entry
            return 0

        lax.fori_loop(0, NBLK, finish_diag, 0)
        bias = jnp.broadcast_to(jnp.log(weight_ref[...]), (8, 128)) - 0.5 * x_ref[x_at(g, 48), :] - constant
        coarse = bias.astype(jnp.bfloat16).astype(jnp.float32)
        w_ref[w_at(g, OFF_BIAS), :] = coarse
        w_ref[w_at(g, OFF_BIAS + 1), :] = bias - coarse
        for n in range(OFF_BIAS + 2, FEATS):
            w_ref[w_at(g, n), :] = zero
        return 0

    lax.fori_loop(0, 2, finish, 0)


def build_products(e_ref, hi_ref, lo_ref):
    width = e_ref.shape[1]
    blocks = [e_ref[i * 8 : i * 8 + 8, :] for i in range(NBLK)]

    def row(i):
        return jnp.broadcast_to(e_ref[i : i + 1, :], (8, width))

    groups = []
    for i in range(NBLK):
        for j in range(i):
            groups += [lambda i=i, j=j, a=a: row(i * 8 + a) * blocks[j] for a in range(8)]
    groups += [lambda j=j: row(48) * blocks[j] for j in range(NBLK)]
    groups += [lambda: row(48) * row(48)]
    for i in range(NBLK):
        for d in range(5):
            groups += [lambda i=i, d=d: blocks[i] * (pltpu.roll(blocks[i], 8 - d, 0) if d else blocks[i])]
    groups += [lambda: jnp.ones((8, width), jnp.float32)]
    groups += [lambda: jnp.zeros((8, width), jnp.float32)] * 2
    for n in range(0, len(groups), 2):
        both = jnp.concatenate([groups[n](), groups[n + 1]()], axis=0)
        head = both.astype(jnp.bfloat16)
        rest = (both - head.astype(jnp.float32)).astype(jnp.bfloat16)
        hi_ref[n * 8 : n * 8 + 16, :] = head
        lo_ref[n * 8 : n * 8 + 16, :] = rest


def prepare(se_ref, index_ref, root_ref, grid_ref, base_ref, level_ref, covar_ref, se2_ref, cov_ref, rows_ref):
    units = root_ref.shape[1]
    for u in range(units):
        root = root_ref[:, u, :]
        cov_ref[u * 56 : u * 56 + R, 0:R] = lax.dot_general(
            root, root, (((1,), (1,)), ((), ())), precision=HIGHEST, preferred_element_type=jnp.float32
        )
    comps = base_ref.shape[1]
    pick = (lax.broadcasted_iota(jnp.int32, (units, comps), 0) == base_ref[...]).astype(jnp.bfloat16)
    scale = jnp.zeros((1, comps), jnp.float32)
    for n in range(grid_ref.shape[0]):
        scale = jnp.where(level_ref[...] == n, grid_ref[n], scale)
    scale2 = scale * scale

    def one_row(i, _):
        part = cov_ref[pl.ds(i, units, stride=56), :].T[0:56]
        total = None
        for _ in range(3):
            head = part.astype(jnp.bfloat16)
            term = jnp.dot(head, pick, preferred_element_type=jnp.float32)
            total = term if total is None else total + term
            part = part - head.astype(jnp.float32)
        covar_ref[i] = total * scale2
        return 0

    lax.fori_loop(0, R, one_row, 0, unroll=7)
    for t in range(index_ref.shape[0]):
        rows_ref[t : t + 1, 0:R] = se_ref[pl.ds(index_ref[t], 1), :]
    squares = rows_ref[...] * rows_ref[...]
    for i in range(R):
        se2_ref[i] = jnp.broadcast_to(squares[:, i : i + 1], se2_ref.shape[1:])


def sweep_kernel(
    se_in, index_in, root_in, grid_in, base_in, level_in, weight_in, w_ref,
    se_ref, index_ref, root_ref, grid_ref, base_ref, level_ref, weight_ref, sems,
    covar_ref, se2_ref, cov_ref, rows_ref, d_ref, b_ref, c_ref, v_ref, x_ref,
):
    sources = (se_in, index_in, root_in, grid_in, base_in, level_in, weight_in)
    places = (se_ref, index_ref, root_ref, grid_ref, base_ref, level_ref, weight_ref)
    copies = [pltpu.make_async_copy(a, b, sems.at[n]) for n, (a, b) in enumerate(zip(sources, places))]
    for copy in copies:
        copy.start()
    for copy in copies:
        copy.wait()
    prepare(se_ref, index_ref, root_ref, grid_ref, base_ref, level_ref, covar_ref, se2_ref, cov_ref, rows_ref)
    invert_all(covar_ref, se2_ref, weight_ref, w_ref, d_ref, b_ref, c_ref, v_ref, x_ref)


def sweep_stage(se_table, se_index, base_root, grid_scale, comp_base, comp_grid, weights):
    tissues = se_table.shape[1]
    units = base_root.shape[0]
    tiles = se_index.shape[0]
    comps = comp_base.shape[0]
    panel = pltpu.VMEM((2 * NBLK * 64 * 8, 128), jnp.float32)
    return pl.pallas_call(
        sweep_kernel,
        in_specs=[pl.BlockSpec(memory_space=pltpu.HBM)] * 7,
        out_specs=pl.BlockSpec(memory_space=pltpu.VMEM),
        out_shape=pltpu.VMEM((2 * FEATS * 8, 128), jnp.float32),
        scratch_shapes=[
            pltpu.VMEM(se_table.shape, jnp.float32),
            pltpu.SMEM((tiles,), jnp.int32),
            pltpu.VMEM((tissues, units, tissues), jnp.float32),
            pltpu.SMEM(grid_scale.shape, jnp.float32),
            pltpu.VMEM((1, comps), jnp.int32),
            pltpu.VMEM((1, comps), jnp.int32),
            pltpu.VMEM((1, comps), jnp.float32),
            pltpu.SemaphoreType.DMA((7,)),
            pltpu.VMEM((R, 56, comps), jnp.float32),
            pltpu.VMEM((R, tiles, comps), jnp.float32),
            pltpu.VMEM((units * 56, 128), jnp.float32),
            pltpu.VMEM((tiles, 128), jnp.float32),
            panel,
            panel,
            panel,
            pltpu.VMEM((2 * 64 * 8, 128), jnp.float32),
            pltpu.VMEM((2 * 72 * 8, 128), jnp.float32),
        ],
        compiler_params=pltpu.CompilerParams(vmem_limit_bytes=32 * 1024 * 1024),
        cost_estimate=pl.CostEstimate(flops=250_000_000, bytes_accessed=60_000_000, transcendentals=0),
        name="sweep",
    )(
        se_table, se_index, base_root.transpose(1, 0, 2), grid_scale,
        comp_base.reshape(1, comps), comp_grid.reshape(1, comps), weights.reshape(1, comps),
    )


def build_tile(t, e_ref, w_ref, hi_ref, lo_ref, left_ref):
    first = (t // 8) * (FEATS * 8) + t % 8
    for n in range(FEATS // 128):
        part = w_ref[pl.ds(first + n * 1024, 128, stride=8), :].T
        head = part.astype(jnp.bfloat16)
        left_ref[0:128, n * 128 : (n + 1) * 128] = head
        left_ref[128:256, n * 128 : (n + 1) * 128] = (part - head.astype(jnp.float32)).astype(jnp.bfloat16)
    build_products(e_ref.at[:, pl.ds(pl.multiple_of(t * TILE, TILE), TILE)], hi_ref, lo_ref)


def score_tile(t, hi_ref, lo_ref, left_ref, scores_ref, stats_ref):
    cols = pl.ds(pl.multiple_of(t * TILE, TILE), TILE)
    main = jnp.dot(left_ref[...], hi_ref[...], preferred_element_type=jnp.float32)
    rest = jnp.dot(left_ref[0:128, :], lo_ref[...], preferred_element_type=jnp.float32)
    scores = main[0:128] + (main[128:256] + rest)
    top = jnp.max(scores, axis=0, keepdims=True)
    scores_ref[:, cols] = scores
    stats_ref[0:1, cols] = top
    stats_ref[1:2, cols] = jnp.sum(jnp.exp(scores - top), axis=0, keepdims=True)


def tile_kernel(
    count, all_pairs, all_comps, e_ref, w_ref, resp_ref, loglik_ref, logw_ref,
    hi_a, lo_a, left_a, hi_b, lo_b, left_b, scores_ref, stats_ref,
    other_ref, mine_ref, slots_ref, pair_sems, send_sems, recv_sems,
):
    chip, core = lax.axis_index("pairs"), lax.axis_index("comp")
    mesh_id = pl.DeviceIdType.MESH
    barrier = pltpu.get_barrier_semaphore()
    pl.semaphore_signal(barrier, inc=1, device_id=(chip, 1 - core), device_id_type=mesh_id)

    def greet(d, _):
        pl.semaphore_signal(barrier, inc=1, device_id=((chip + d) % count, core), device_id_type=mesh_id)
        return 0

    lax.fori_loop(1, count, greet, 0)
    tiles = e_ref.shape[1] // TILE
    build_tile(0, e_ref, w_ref, hi_a, lo_a, left_a)

    def two_tiles(s, _):
        score_tile(2 * s, hi_a, lo_a, left_a, scores_ref, stats_ref)
        build_tile(2 * s + 1, e_ref, w_ref, hi_b, lo_b, left_b)
        score_tile(2 * s + 1, hi_b, lo_b, left_b, scores_ref, stats_ref)
        build_tile((2 * s + 2) % tiles, e_ref, w_ref, hi_a, lo_a, left_a)
        return 0

    lax.fori_loop(0, tiles // 2, two_tiles, 0)
    pl.semaphore_wait(barrier, count)
    swap = pltpu.make_async_remote_copy(
        src_ref=stats_ref, dst_ref=other_ref, send_sem=pair_sems.at[0], recv_sem=pair_sems.at[1],
        device_id=(chip, 1 - core), device_id_type=mesh_id,
    )
    swap.start()
    swap.wait()

    def one_part(n, mass):
        cols = pl.ds(pl.multiple_of(n * TILE, TILE), TILE)
        m0, m1 = stats_ref[0:1, cols], other_ref[0:1, cols]
        top = jnp.maximum(m0, m1)
        total = stats_ref[1:2, cols] * jnp.exp(m0 - top) + other_ref[1:2, cols] * jnp.exp(m1 - top)
        loglik = top + jnp.log(total)
        loglik_ref[0:1, cols] = loglik
        resp = jnp.exp(scores_ref[:, cols] - loglik)
        resp_ref[:, cols] = resp
        for j in range(TILE // 128):
            mass = mass + resp[:, j * 128 : (j + 1) * 128]
        return mass

    mass = lax.fori_loop(0, tiles, one_part, jnp.zeros((128, 128), jnp.float32))
    own = jnp.sum(mass.T, axis=0, keepdims=True)
    mine_ref[...] = own
    slots_ref[chip] = own

    def copy_to(peer, slot):
        return pltpu.make_async_remote_copy(
            src_ref=mine_ref, dst_ref=slots_ref.at[slot], send_sem=send_sems.at[peer], recv_sem=recv_sems.at[slot],
            device_id=(peer, core), device_id_type=mesh_id,
        )

    def send(d, _):
        copy_to((chip + d) % count, chip).start()
        return 0

    lax.fori_loop(1, count, send, 0)

    def receive(d, _):
        peer = (chip + d) % count
        copy_to(peer, peer).wait_recv()
        return 0

    lax.fori_loop(1, count, receive, 0)
    parts = [slots_ref[n] for n in range(count)]
    while len(parts) > 1:
        parts = [parts[n] + parts[n + 1] for n in range(0, len(parts), 2)]
    logw_ref[...] = jnp.log((parts[0] + 1.0) / (all_pairs + all_comps))

    def sent(d, _):
        copy_to((chip + d) % count, chip).wait_send()
        return 0

    lax.fori_loop(1, count, sent, 0)


def write_kernel(resp_ref, loglik_ref, logw_ref, resp_out, loglik_out, logw_out, sems):
    pairs = ((resp_ref, resp_out), (loglik_ref, loglik_out), (logw_ref, logw_out))
    copies = [pltpu.make_async_copy(a, b, sems.at[n]) for n, (a, b) in enumerate(pairs)]
    for copy in copies:
        copy.start()
    for copy in copies:
        copy.wait()


def per_device(effects, se_table, se_index, base_root, grid_scale, comp_base, comp_grid, weights):
    pairs = effects.shape[1]
    comps = comp_base.shape[0]
    w = sweep_stage(se_table, se_index, base_root, grid_scale, comp_base, comp_grid, weights)
    count = lax.axis_size("pairs")
    vmem = pl.BlockSpec(memory_space=pltpu.VMEM)
    products = [
        pltpu.VMEM((FEATS, TILE), jnp.bfloat16),
        pltpu.VMEM((FEATS, TILE), jnp.bfloat16),
        pltpu.VMEM((256, FEATS), jnp.bfloat16),
    ]
    shapes = ((comps, pairs), (1, pairs), (1, comps))
    results = pl.pallas_call(
        functools.partial(tile_kernel, count, pairs * count, comps * lax.axis_size("comp")),
        in_specs=[vmem, vmem],
        out_specs=[vmem, vmem, vmem],
        out_shape=[pltpu.VMEM(shape, jnp.float32) for shape in shapes],
        scratch_shapes=products + products + [
            pltpu.VMEM((comps, pairs), jnp.float32),
            pltpu.VMEM((2, pairs), jnp.float32),
            pltpu.VMEM((2, pairs), jnp.float32),
            pltpu.VMEM((1, comps), jnp.float32),
            pltpu.VMEM((count, 1, comps), jnp.float32),
            pltpu.SemaphoreType.DMA((2,)),
            pltpu.SemaphoreType.DMA((count,)),
            pltpu.SemaphoreType.DMA((count,)),
        ],
        compiler_params=pltpu.CompilerParams(
            collective_id=0, has_side_effects=True, vmem_limit_bytes=24 * 1024 * 1024
        ),
        name="tiles",
    )(effects, w)
    resp, loglik, logw = pl.pallas_call(
        write_kernel,
        in_specs=[vmem, vmem, vmem],
        out_specs=[pl.BlockSpec(memory_space=pltpu.HBM)] * 3,
        out_shape=[jax.ShapeDtypeStruct(shape, jnp.float32) for shape in shapes],
        scratch_shapes=[pltpu.SemaphoreType.DMA((3,))],
        compiler_params=pltpu.CompilerParams(vmem_limit_bytes=4 * 1024 * 1024),
        name="write",
    )(*results)
    return (resp, logw.reshape(comps), loglik.reshape(pairs))


def solution(mesh):
    placed = (P(None, "pairs"), P(), P("pairs"), P(), P(), P("comp"), P("comp"), P("comp"))
    return jax.shard_map(
        per_device,
        mesh=mesh,
        in_specs=placed,
        out_specs=(P("comp", "pairs"), P("comp"), P("pairs")),
        check_vma=False,
    )
```

```python
import functools
import math

import jax
import jax.numpy as jnp
from jax import lax
from jax.experimental import pallas as pl
from jax.experimental.pallas import tpu as pltpu
from jax.sharding import PartitionSpec as P

TILE = 512
R = 49
NBLK = 6
FEATS = 1280
OFF_BORDER = 960
OFF_LAST = 1008
OFF_DIAG = 1016
OFF_BIAS = 1256
HIGHEST = lax.Precision.HIGHEST


def row8(index):
    return pl.ds(pl.multiple_of(index * 8, 8), 8)


def invert_all(covar_ref, se2_ref, weight_ref, w_ref, d_ref, b_ref, c_ref, v_ref, x_ref):
    def w_at(g, f):
        return row8(g * FEATS + f)

    def d_at(g, block, a, c):
        return row8((g * NBLK + block) * 64 + a * 8 + c)

    def p_at(g, block, a, c):
        return row8((g * NBLK + block) * 64 + a * 8 + c)

    def pair_base(i, j):
        return (i * (i - 1) // 2 + j) * 64

    def cov(i, j):
        return jnp.broadcast_to(covar_ref[i, pl.ds(j, 1), :], (8, 128))

    def x_at(g, n):
        return row8(g * 72 + n)

    for g in range(2):
        se_last = se2_ref[48, g * 8 : g * 8 + 8, :]
        pivot = cov(48, 48) + se_last
        inv = 1.0 / pivot
        x_ref[x_at(g, 48), :] = jnp.log(pivot)
        w_ref[w_at(g, OFF_LAST), :] = -inv
        for i in range(48):
            edge = cov(48, i)
            x_ref[x_at(g, i), :] = edge
            w_ref[w_at(g, OFF_BORDER + i), :] = edge * inv

    def init_group(g, _):
        def init_row(i, _):
            edges = [x_ref[x_at(g, i * 8 + a), :] for a in range(8)]

            def init_pair(j, _):
                scaled = [w_ref[w_at(g, OFF_BORDER + j * 8 + c), :] for c in range(8)]
                base = pair_base(i, j)
                for a in range(8):
                    for c in range(8):
                        w_ref[w_at(g, base + a * 8 + c), :] = cov(i * 8 + a, j * 8 + c) - edges[a] * scaled[c]
                return 0

            lax.fori_loop(0, i, init_pair, 0)
            scaled = [w_ref[w_at(g, OFF_BORDER + i * 8 + c), :] for c in range(8)]
            for a in range(8):
                for c in range(a + 1):
                    entry = cov(i * 8 + a, i * 8 + c) - edges[a] * scaled[c]
                    if a == c:
                        entry = entry + se2_ref[i * 8 + a, pl.ds(pl.multiple_of(g * 8, 8), 8), :]
                    d_ref[d_at(g, i, a, c), :] = entry
            return 0

        lax.fori_loop(0, NBLK, init_row, 0)
        return 0

    lax.fori_loop(0, 2, init_group, 0)

    def pivot_block(k):
        for g in range(2):
            m = {(a, c): d_ref[d_at(g, k, a, c), :] for a in range(8) for c in range(a + 1)}
            product = None
            for s in range(8):
                p = m[s, s]
                product = p if product is None else product * p
                inv = 1.0 / p
                col = {a: (m[a, s] if a > s else m[s, a]) for a in range(8) if a != s}
                scaled = {a: col[a] * inv for a in col}
                for a in col:
                    for c in col:
                        if c <= a:
                            m[a, c] = m[a, c] - scaled[a] * col[c]
                for a in col:
                    m[max(a, s), min(a, s)] = scaled[a]
                m[s, s] = -inv
            x_ref[x_at(g, 48), :] = x_ref[x_at(g, 48), :] + jnp.log(product)
            for a in range(8):
                for c in range(8):
                    entry = m[max(a, c), min(a, c)]
                    if c <= a:
                        d_ref[d_at(g, k, a, c), :] = entry
                    v_ref[row8(g * 64 + a * 8 + c), :] = -entry

    def scale_block(g, k, j, swap):
        base = pair_base(k, j) if swap else pair_base(j, k)
        for half in range(2):
            rows = range(half * 4, half * 4 + 4)
            acc = {}
            for l in range(8):
                left = {}
                for a in rows:
                    left[a] = w_ref[w_at(g, base + (l * 8 + a if swap else a * 8 + l)), :]
                    c_ref[p_at(g, j, a, l), :] = left[a]
                for c in range(8):
                    right = v_ref[row8(g * 64 + l * 8 + c), :]
                    for a in rows:
                        term = left[a] * right
                        acc[a, c] = term if l == 0 else acc[a, c] + term
            for a in rows:
                for c in range(8):
                    b_ref[p_at(g, j, a, c), :] = acc[a, c]
        for a in range(8):
            for c in range(8):
                w_ref[w_at(g, base + (c * 8 + a if swap else a * 8 + c)), :] = b_ref[p_at(g, j, a, c), :]

    def scale_border(g, k):
        old = [w_ref[w_at(g, OFF_BORDER + k * 8 + m), :] for m in range(8)]
        total = w_ref[w_at(g, OFF_LAST), :]
        for c in range(8):
            new = old[0] * v_ref[row8(g * 64 + c), :]
            for l in range(1, 8):
                new = new + old[l] * v_ref[row8(g * 64 + l * 8 + c), :]
            x_ref[x_at(g, 49 + c), :] = new
            w_ref[w_at(g, OFF_BORDER + k * 8 + c), :] = new
            total = total - new * old[c]
        w_ref[w_at(g, OFF_LAST), :] = total

    def update_pair(g, i, j):
        base = pair_base(i, j)
        for half in range(2):
            rows = range(half * 4, half * 4 + 4)
            acc = {(a, c): w_ref[w_at(g, base + a * 8 + c), :] for a in rows for c in range(8)}
            for m in range(8):
                left = {a: b_ref[p_at(g, i, a, m), :] for a in rows}
                for c in range(8):
                    right = c_ref[p_at(g, j, c, m), :]
                    for a in rows:
                        acc[a, c] = acc[a, c] - left[a] * right
            for a in rows:
                for c in range(8):
                    w_ref[w_at(g, base + a * 8 + c), :] = acc[a, c]

    def update_diag(g, i):
        for rows in (range(0, 6), range(6, 8)):
            acc = {(a, c): d_ref[d_at(g, i, a, c), :] for a in rows for c in range(a + 1)}
            if rows[0]:
                edge = [w_ref[w_at(g, OFF_BORDER + i * 8 + c), :] for c in range(8)]
            for m in range(8):
                left = {a: b_ref[p_at(g, i, a, m), :] for a in rows}
                if rows[0]:
                    last = x_ref[x_at(g, 49 + m), :]
                for c in range(rows[-1] + 1):
                    right = c_ref[p_at(g, i, c, m), :]
                    for a in rows:
                        if c <= a:
                            acc[a, c] = acc[a, c] - left[a] * right
                    if rows[0]:
                        edge[c] = edge[c] - last * right
            for a, c in acc:
                d_ref[d_at(g, i, a, c), :] = acc[a, c]
            if rows[0]:
                for c in range(8):
                    w_ref[w_at(g, OFF_BORDER + i * 8 + c), :] = edge[c]

    def sweep(k, _):
        pivot_block(k)

        def scale_one(j, swap):
            for g in range(2):
                scale_block(g, k, j, swap)

        lax.fori_loop(0, k, lambda j, z: (scale_one(j, True), z)[1], 0)
        lax.fori_loop(k + 1, NBLK, lambda j, z: (scale_one(j, False), z)[1], 0)
        for g in range(2):
            scale_border(g, k)

        def update_row(t, _):
            i = t + (t >= k).astype(jnp.int32)

            def update_one(s, _):
                for g in range(2):
                    update_pair(g, i, s + (s >= k).astype(jnp.int32))
                return 0

            lax.fori_loop(0, t, update_one, 0)
            for g in range(2):
                update_diag(g, i)
            return 0

        lax.fori_loop(0, NBLK - 1, update_row, 0)
        return 0

    lax.fori_loop(0, NBLK, sweep, 0)

    zero = jnp.zeros((8, 128), jnp.float32)
    constant = 0.5 * R * math.log(2.0 * math.pi)

    def finish(g, _):
        w_ref[w_at(g, OFF_LAST), :] = 0.5 * w_ref[w_at(g, OFF_LAST), :]
        for n in range(1, 8):
            w_ref[w_at(g, OFF_LAST + n), :] = zero

        def finish_diag(i, _):
            for d in range(5):
                weight = 1.0 if 0 < d < 4 else 0.5
                for c in range(8):
                    a = (c + d) % 8
                    entry = d_ref[d_at(g, i, max(a, c), min(a, c)), :]
                    w_ref[w_at(g, OFF_DIAG + i * 40 + d * 8 + c), :] = weight * entry
            return 0

        lax.fori_loop(0, NBLK, finish_diag, 0)
        bias = jnp.broadcast_to(jnp.log(weight_ref[...]), (8, 128)) - 0.5 * x_ref[x_at(g, 48), :] - constant
        coarse = bias.astype(jnp.bfloat16).astype(jnp.float32)
        w_ref[w_at(g, OFF_BIAS), :] = coarse
        w_ref[w_at(g, OFF_BIAS + 1), :] = bias - coarse
        for n in range(OFF_BIAS + 2, FEATS):
            w_ref[w_at(g, n), :] = zero
        return 0

    lax.fori_loop(0, 2, finish, 0)


def product_groups(e_ref):
    width = e_ref.shape[1]

    def block(i):
        return e_ref[i * 8 : i * 8 + 8, :]

    def row(i):
        return jnp.broadcast_to(e_ref[i : i + 1, :], (8, width))

    groups = []
    for i in range(NBLK):
        for j in range(i):
            groups += [lambda i=i, j=j, a=a: row(i * 8 + a) * block(j) for a in range(8)]
    groups += [lambda j=j: row(48) * block(j) for j in range(NBLK)]
    groups += [lambda: row(48) * row(48)]
    for i in range(NBLK):
        for d in range(5):
            groups += [lambda i=i, d=d: block(i) * (pltpu.roll(block(i), 8 - d, 0) if d else block(i))]
    groups += [lambda: jnp.ones((8, width), jnp.float32)]
    groups += [lambda: jnp.zeros((8, width), jnp.float32)] * 2
    return groups


def prepare(se_ref, index_ref, root_ref, grid_ref, base_ref, level_ref, covar_ref, se2_ref, cov_ref, rows_ref):
    units = root_ref.shape[1]
    for u in range(units):
        root = root_ref[:, u, :]
        cov_ref[u * 56 : u * 56 + R, 0:R] = lax.dot_general(
            root, root, (((1,), (1,)), ((), ())), precision=HIGHEST, preferred_element_type=jnp.float32
        )
    comps = base_ref.shape[1]
    pick = (lax.broadcasted_iota(jnp.int32, (units, comps), 0) == base_ref[...]).astype(jnp.bfloat16)
    scale = jnp.zeros((1, comps), jnp.float32)
    for n in range(grid_ref.shape[0]):
        scale = jnp.where(level_ref[...] == n, grid_ref[n], scale)
    scale2 = scale * scale

    def one_row(i, _):
        part = cov_ref[pl.ds(i, units, stride=56), :].T[0:56]
        total = None
        for _ in range(3):
            head = part.astype(jnp.bfloat16)
            term = jnp.dot(head, pick, preferred_element_type=jnp.float32)
            total = term if total is None else total + term
            part = part - head.astype(jnp.float32)
        covar_ref[i] = total * scale2
        return 0

    lax.fori_loop(0, R, one_row, 0, unroll=7)
    for t in range(index_ref.shape[0]):
        rows_ref[t : t + 1, 0:R] = se_ref[pl.ds(index_ref[t], 1), :]
    squares = rows_ref[...] * rows_ref[...]
    for i in range(R):
        se2_ref[i] = jnp.broadcast_to(squares[:, i : i + 1], se2_ref.shape[1:])


def sweep_kernel(
    se_in, index_in, root_in, grid_in, base_in, level_in, weight_in, w_ref,
    se_ref, index_ref, root_ref, grid_ref, base_ref, level_ref, weight_ref, sems,
    covar_ref, se2_ref, cov_ref, rows_ref, d_ref, b_ref, c_ref, v_ref, x_ref,
):
    sources = (se_in, index_in, root_in, grid_in, base_in, level_in, weight_in)
    places = (se_ref, index_ref, root_ref, grid_ref, base_ref, level_ref, weight_ref)
    copies = [pltpu.make_async_copy(a, b, sems.at[n]) for n, (a, b) in enumerate(zip(sources, places))]
    for copy in copies:
        copy.start()
    for copy in copies:
        copy.wait()
    prepare(se_ref, index_ref, root_ref, grid_ref, base_ref, level_ref, covar_ref, se2_ref, cov_ref, rows_ref)
    invert_all(covar_ref, se2_ref, weight_ref, w_ref, d_ref, b_ref, c_ref, v_ref, x_ref)


def sweep_stage(se_table, se_index, base_root, grid_scale, comp_base, comp_grid, weights):
    tissues = se_table.shape[1]
    units = base_root.shape[0]
    tiles = se_index.shape[0]
    comps = comp_base.shape[0]
    panel = pltpu.VMEM((2 * NBLK * 64 * 8, 128), jnp.float32)
    operands = (
        se_table, se_index, base_root.transpose(1, 0, 2), grid_scale,
        comp_base.reshape(1, comps), comp_grid.reshape(1, comps), weights.reshape(1, comps),
    )
    return pl.pallas_call(
        sweep_kernel,
        in_specs=[pl.BlockSpec(memory_space=pltpu.HBM)] * 7,
        out_specs=pl.BlockSpec(memory_space=pltpu.VMEM),
        out_shape=pltpu.VMEM((2 * FEATS * 8, 128), jnp.float32),
        scratch_shapes=[
            pltpu.VMEM(se_table.shape, jnp.float32),
            pltpu.SMEM((tiles,), jnp.int32),
            pltpu.VMEM((tissues, units, tissues), jnp.float32),
            pltpu.SMEM(grid_scale.shape, jnp.float32),
            pltpu.VMEM((1, comps), jnp.int32),
            pltpu.VMEM((1, comps), jnp.int32),
            pltpu.VMEM((1, comps), jnp.float32),
            pltpu.SemaphoreType.DMA((7,)),
            pltpu.VMEM((R, 56, comps), jnp.float32),
            pltpu.VMEM((R, tiles, comps), jnp.float32),
            pltpu.VMEM((units * 56, 128), jnp.float32),
            pltpu.VMEM((tiles, 128), jnp.float32),
            panel,
            panel,
            panel,
            pltpu.VMEM((2 * 64 * 8, 128), jnp.float32),
            pltpu.VMEM((2 * 72 * 8, 128), jnp.float32),
        ],
        compiler_params=pltpu.CompilerParams(vmem_limit_bytes=32 * 1024 * 1024),
        cost_estimate=pl.CostEstimate(flops=250_000_000, bytes_accessed=60_000_000, transcendentals=0),
        name="sweep",
    )(*(pltpu.with_memory_space_constraint(operand, pltpu.HBM) for operand in operands))


def build_chunk(t, chunk, e_ref, w_ref, hi_ref, lo_ref, left_ref):
    first = (t // 8) * (FEATS * 8) + t % 8
    for n in (2 * chunk, 2 * chunk + 1):
        part = w_ref[pl.ds(first + n * 1024, 128, stride=8), :].T
        head = part.astype(jnp.bfloat16)
        left_ref[0:128, n * 128 : (n + 1) * 128] = head
        left_ref[128:256, n * 128 : (n + 1) * 128] = (part - head.astype(jnp.float32)).astype(jnp.bfloat16)
    groups = product_groups(e_ref.at[:, pl.ds(pl.multiple_of(t * TILE, TILE), TILE)])
    for n in range(chunk * 32, chunk * 32 + 32, 2):
        both = jnp.concatenate([groups[n](), groups[n + 1]()], axis=0)
        head = both.astype(jnp.bfloat16)
        rest = (both - head.astype(jnp.float32)).astype(jnp.bfloat16)
        hi_ref[n * 8 : n * 8 + 16, :] = head
        lo_ref[n * 8 : n * 8 + 16, :] = rest


def score_and_build(t, now, later, following, e_ref, w_ref, scores_ref, stats_ref):
    hi_ref, lo_ref, left_ref = now
    scores = None
    for chunk in range(FEATS // 256):
        rows = slice(chunk * 256, chunk * 256 + 256)
        main = jnp.dot(left_ref[:, rows], hi_ref[rows, :], preferred_element_type=jnp.float32)
        rest = jnp.dot(left_ref[0:128, rows], lo_ref[rows, :], preferred_element_type=jnp.float32)
        part = main[0:128] + (main[128:256] + rest)
        scores = part if scores is None else scores + part
        build_chunk(later, chunk, e_ref, w_ref, *following)
    cols = pl.ds(pl.multiple_of(t * TILE, TILE), TILE)
    top = jnp.max(scores, axis=0, keepdims=True)
    scores_ref[:, cols] = scores
    stats_ref[0:1, cols] = top
    stats_ref[1:2, cols] = jnp.sum(jnp.exp(scores - top), axis=0, keepdims=True)


def tile_kernel(
    count, all_pairs, all_comps, e_ref, w_ref, resp_ref, loglik_ref, logw_ref,
    hi_a, lo_a, left_a, hi_b, lo_b, left_b, scores_ref, stats_ref,
    other_ref, mine_ref, slots_ref, pair_sems, mass_sems,
):
    chip, core = lax.axis_index("pairs"), lax.axis_index("comp")
    mesh_id = pl.DeviceIdType.MESH
    barrier = pltpu.get_barrier_semaphore()
    pl.semaphore_signal(barrier, inc=1, device_id=(chip, 1 - core), device_id_type=mesh_id)

    def greet(d, _):
        pl.semaphore_signal(barrier, inc=1, device_id=((chip + d) % count, core), device_id_type=mesh_id)
        return 0

    lax.fori_loop(1, count, greet, 0)
    tiles = e_ref.shape[1] // TILE
    one, two = (hi_a, lo_a, left_a), (hi_b, lo_b, left_b)
    for chunk in range(FEATS // 256):
        build_chunk(0, chunk, e_ref, w_ref, *one)

    def two_tiles(s, _):
        score_and_build(2 * s, one, 2 * s + 1, two, e_ref, w_ref, scores_ref, stats_ref)
        score_and_build(2 * s + 1, two, (2 * s + 2) % tiles, one, e_ref, w_ref, scores_ref, stats_ref)
        return 0

    lax.fori_loop(0, tiles // 2, two_tiles, 0)
    pl.semaphore_wait(barrier, count)
    swap = pltpu.make_async_remote_copy(
        src_ref=stats_ref, dst_ref=other_ref, send_sem=pair_sems.at[0], recv_sem=pair_sems.at[1],
        device_id=(chip, 1 - core), device_id_type=mesh_id,
    )
    swap.start()
    swap.wait()

    def one_part(n, mass):
        cols = pl.ds(pl.multiple_of(n * TILE, TILE), TILE)
        m0, m1 = stats_ref[0:1, cols], other_ref[0:1, cols]
        top = jnp.maximum(m0, m1)
        total = stats_ref[1:2, cols] * jnp.exp(m0 - top) + other_ref[1:2, cols] * jnp.exp(m1 - top)
        loglik = top + jnp.log(total)
        loglik_ref[0:1, cols] = loglik
        resp = jnp.exp(scores_ref[:, cols] - loglik)
        resp_ref[:, cols] = resp
        for j in range(TILE // 128):
            mass = mass + resp[:, j * 128 : (j + 1) * 128]
        return mass

    mass = lax.fori_loop(0, tiles, one_part, jnp.zeros((128, 128), jnp.float32))
    own = jnp.sum(mass.T, axis=0, keepdims=True)
    mine_ref[...] = own
    slots_ref[chip] = own

    def send(n, _):
        far = 1 + (n + (2 * count) // 3 - 1) % (count - 1)
        pltpu.make_async_remote_copy(
            src_ref=mine_ref, dst_ref=slots_ref.at[chip], send_sem=mass_sems.at[0], recv_sem=mass_sems.at[1],
            device_id=((chip + far) % count, core), device_id_type=mesh_id,
        ).start()
        return 0

    lax.fori_loop(0, count - 1, send, 0)
    every = pltpu.make_async_remote_copy(
        src_ref=slots_ref.at[pl.ds(0, count - 1)], dst_ref=slots_ref.at[pl.ds(0, count - 1)],
        send_sem=mass_sems.at[0], recv_sem=mass_sems.at[1],
        device_id=((chip + 1) % count, core), device_id_type=mesh_id,
    )
    every.wait_recv()
    parts = [slots_ref[n] for n in range(count)]
    while len(parts) > 1:
        parts = [parts[n] + parts[n + 1] for n in range(0, len(parts), 2)]
    logw_ref[...] = jnp.log((parts[0] + 1.0) / (all_pairs + all_comps))
    every.wait_send()


def write_kernel(resp_ref, loglik_ref, logw_ref, resp_out, loglik_out, logw_out, sems):
    pairs = ((resp_ref, resp_out), (loglik_ref, loglik_out), (logw_ref, logw_out))
    copies = [pltpu.make_async_copy(a, b, sems.at[n]) for n, (a, b) in enumerate(pairs)]
    for copy in copies:
        copy.start()
    for copy in copies:
        copy.wait()


def per_device(effects, se_table, se_index, base_root, grid_scale, comp_base, comp_grid, weights):
    pairs = effects.shape[1]
    comps = comp_base.shape[0]
    w = sweep_stage(se_table, se_index, base_root, grid_scale, comp_base, comp_grid, weights)
    count = lax.axis_size("pairs")
    vmem = pl.BlockSpec(memory_space=pltpu.VMEM)
    products = [
        pltpu.VMEM((FEATS, TILE), jnp.bfloat16),
        pltpu.VMEM((FEATS, TILE), jnp.bfloat16),
        pltpu.VMEM((256, FEATS), jnp.bfloat16),
    ]
    shapes = ((comps, pairs), (1, pairs), (1, comps))
    results = pl.pallas_call(
        functools.partial(tile_kernel, count, pairs * count, comps * lax.axis_size("comp")),
        in_specs=[vmem, vmem],
        out_specs=[vmem, vmem, vmem],
        out_shape=[pltpu.VMEM(shape, jnp.float32) for shape in shapes],
        scratch_shapes=products + products + [
            pltpu.VMEM((comps, pairs), jnp.float32),
            pltpu.VMEM((2, pairs), jnp.float32),
            pltpu.VMEM((2, pairs), jnp.float32),
            pltpu.VMEM((1, comps), jnp.float32),
            pltpu.VMEM((count, 1, comps), jnp.float32),
            pltpu.SemaphoreType.DMA((2,)),
            pltpu.SemaphoreType.DMA((2,)),
        ],
        compiler_params=pltpu.CompilerParams(
            collective_id=0, has_side_effects=True, vmem_limit_bytes=24 * 1024 * 1024,
        ),
        name="tiles",
    )(effects, w)
    resp, loglik, logw = pl.pallas_call(
        write_kernel,
        in_specs=[vmem, vmem, vmem],
        out_specs=[pl.BlockSpec(memory_space=pltpu.HBM)] * 3,
        out_shape=[jax.ShapeDtypeStruct(shape, jnp.float32) for shape in shapes],
        scratch_shapes=[pltpu.SemaphoreType.DMA((3,))],
        compiler_params=pltpu.CompilerParams(vmem_limit_bytes=4 * 1024 * 1024),
        name="write",
    )(*results)
    return (resp, logw.reshape(comps), loglik.reshape(pairs))


def solution(mesh):
    placed = (P(None, "pairs"), P(), P("pairs"), P(), P(), P("comp"), P("comp"), P("comp"))
    return jax.shard_map(
        per_device,
        mesh=mesh,
        in_specs=placed,
        out_specs=(P("comp", "pairs"), P("comp"), P("pairs")),
        check_vma=False,
    )
```

```python
import functools
import math

import jax
import jax.numpy as jnp
from jax import lax
from jax.experimental import pallas as pl
from jax.experimental.pallas import tpu as pltpu
from jax.sharding import PartitionSpec as P

TILE = 512
R = 49
NBLK = 6
FEATS = 1280
OFF_BORDER = 960
OFF_LAST = 1008
OFF_DIAG = 1016
OFF_BIAS = 1256
HIGHEST = lax.Precision.HIGHEST


def row8(index):
    return pl.ds(pl.multiple_of(index * 8, 8), 8)


def invert_all(covar_ref, se2_ref, weight_ref, w_ref, d_ref, b_ref, c_ref, v_ref, x_ref):
    def w_at(g, f):
        return row8(g * FEATS + f)

    def d_at(g, block, a, c):
        return row8((g * NBLK + block) * 64 + a * 8 + c)

    def p_at(g, block, a, c):
        return row8((g * NBLK + block) * 64 + a * 8 + c)

    def pair_base(i, j):
        return (i * (i - 1) // 2 + j) * 64

    def cov(i, j):
        return jnp.broadcast_to(covar_ref[i, pl.ds(j, 1), :], (8, 128))

    def x_at(g, n):
        return row8(g * 72 + n)

    for g in range(2):
        se_last = se2_ref[48, g * 8 : g * 8 + 8, :]
        pivot = cov(48, 48) + se_last
        inv = 1.0 / pivot
        x_ref[x_at(g, 48), :] = jnp.log(pivot)
        w_ref[w_at(g, OFF_LAST), :] = -inv
        for i in range(48):
            edge = cov(48, i)
            x_ref[x_at(g, i), :] = edge
            w_ref[w_at(g, OFF_BORDER + i), :] = edge * inv

    def init_group(g, _):
        def init_row(i, _):
            edges = [x_ref[x_at(g, i * 8 + a), :] for a in range(8)]

            def init_pair(j, _):
                scaled = [w_ref[w_at(g, OFF_BORDER + j * 8 + c), :] for c in range(8)]
                base = pair_base(i, j)
                for a in range(8):
                    for c in range(8):
                        w_ref[w_at(g, base + a * 8 + c), :] = cov(i * 8 + a, j * 8 + c) - edges[a] * scaled[c]
                return 0

            lax.fori_loop(0, i, init_pair, 0)
            scaled = [w_ref[w_at(g, OFF_BORDER + i * 8 + c), :] for c in range(8)]
            for a in range(8):
                for c in range(a + 1):
                    entry = cov(i * 8 + a, i * 8 + c) - edges[a] * scaled[c]
                    if a == c:
                        entry = entry + se2_ref[i * 8 + a, pl.ds(pl.multiple_of(g * 8, 8), 8), :]
                    d_ref[d_at(g, i, a, c), :] = entry
            return 0

        lax.fori_loop(0, NBLK, init_row, 0)
        return 0

    lax.fori_loop(0, 2, init_group, 0)

    def pivot_block(k):
        for g in range(2):
            m = {(a, c): d_ref[d_at(g, k, a, c), :] for a in range(8) for c in range(a + 1)}
            product = None
            for s in range(8):
                p = m[s, s]
                product = p if product is None else product * p
                inv = 1.0 / p
                col = {a: (m[a, s] if a > s else m[s, a]) for a in range(8) if a != s}
                scaled = {a: col[a] * inv for a in col}
                for a in col:
                    for c in col:
                        if c <= a:
                            m[a, c] = m[a, c] - scaled[a] * col[c]
                for a in col:
                    m[max(a, s), min(a, s)] = scaled[a]
                m[s, s] = -inv
            x_ref[x_at(g, 48), :] = x_ref[x_at(g, 48), :] + jnp.log(product)
            for a in range(8):
                for c in range(8):
                    entry = m[max(a, c), min(a, c)]
                    if c <= a:
                        d_ref[d_at(g, k, a, c), :] = entry
                    v_ref[row8(g * 64 + a * 8 + c), :] = -entry

    def scale_block(g, k, j, swap):
        base = pair_base(k, j) if swap else pair_base(j, k)
        for half in range(2):
            rows = range(half * 4, half * 4 + 4)
            acc = {}
            for l in range(8):
                left = {}
                for a in rows:
                    left[a] = w_ref[w_at(g, base + (l * 8 + a if swap else a * 8 + l)), :]
                    c_ref[p_at(g, j, a, l), :] = left[a]
                for c in range(8):
                    right = v_ref[row8(g * 64 + l * 8 + c), :]
                    for a in rows:
                        term = left[a] * right
                        acc[a, c] = term if l == 0 else acc[a, c] + term
            for a in rows:
                for c in range(8):
                    b_ref[p_at(g, j, a, c), :] = acc[a, c]
        for a in range(8):
            for c in range(8):
                w_ref[w_at(g, base + (c * 8 + a if swap else a * 8 + c)), :] = b_ref[p_at(g, j, a, c), :]

    def scale_border(g, k):
        old = [w_ref[w_at(g, OFF_BORDER + k * 8 + m), :] for m in range(8)]
        total = w_ref[w_at(g, OFF_LAST), :]
        for c in range(8):
            new = old[0] * v_ref[row8(g * 64 + c), :]
            for l in range(1, 8):
                new = new + old[l] * v_ref[row8(g * 64 + l * 8 + c), :]
            x_ref[x_at(g, 49 + c), :] = new
            w_ref[w_at(g, OFF_BORDER + k * 8 + c), :] = new
            total = total - new * old[c]
        w_ref[w_at(g, OFF_LAST), :] = total

    def update_pair(g, i, j):
        base = pair_base(i, j)
        for half in range(2):
            rows = range(half * 4, half * 4 + 4)
            acc = {(a, c): w_ref[w_at(g, base + a * 8 + c), :] for a in rows for c in range(8)}
            for m in range(8):
                left = {a: b_ref[p_at(g, i, a, m), :] for a in rows}
                for c in range(8):
                    right = c_ref[p_at(g, j, c, m), :]
                    for a in rows:
                        acc[a, c] = acc[a, c] - left[a] * right
            for a in rows:
                for c in range(8):
                    w_ref[w_at(g, base + a * 8 + c), :] = acc[a, c]

    def update_diag(g, i):
        for rows in (range(0, 6), range(6, 8)):
            acc = {(a, c): d_ref[d_at(g, i, a, c), :] for a in rows for c in range(a + 1)}
            if rows[0]:
                edge = [w_ref[w_at(g, OFF_BORDER + i * 8 + c), :] for c in range(8)]
            for m in range(8):
                left = {a: b_ref[p_at(g, i, a, m), :] for a in rows}
                if rows[0]:
                    last = x_ref[x_at(g, 49 + m), :]
                for c in range(rows[-1] + 1):
                    right = c_ref[p_at(g, i, c, m), :]
                    for a in rows:
                        if c <= a:
                            acc[a, c] = acc[a, c] - left[a] * right
                    if rows[0]:
                        edge[c] = edge[c] - last * right
            for a, c in acc:
                d_ref[d_at(g, i, a, c), :] = acc[a, c]
            if rows[0]:
                for c in range(8):
                    w_ref[w_at(g, OFF_BORDER + i * 8 + c), :] = edge[c]

    def sweep(k, _):
        pivot_block(k)

        def scale_one(j, swap):
            for g in range(2):
                scale_block(g, k, j, swap)

        lax.fori_loop(0, k, lambda j, z: (scale_one(j, True), z)[1], 0)
        lax.fori_loop(k + 1, NBLK, lambda j, z: (scale_one(j, False), z)[1], 0)
        for g in range(2):
            scale_border(g, k)

        def update_row(t, _):
            i = t + (t >= k).astype(jnp.int32)

            def update_one(s, _):
                for g in range(2):
                    update_pair(g, i, s + (s >= k).astype(jnp.int32))
                return 0

            lax.fori_loop(0, t, update_one, 0)
            for g in range(2):
                update_diag(g, i)
            return 0

        lax.fori_loop(0, NBLK - 1, update_row, 0)
        return 0

    lax.fori_loop(0, NBLK, sweep, 0)

    zero = jnp.zeros((8, 128), jnp.float32)
    constant = 0.5 * R * math.log(2.0 * math.pi)

    def finish(g, _):
        w_ref[w_at(g, OFF_LAST), :] = 0.5 * w_ref[w_at(g, OFF_LAST), :]
        for n in range(1, 8):
            w_ref[w_at(g, OFF_LAST + n), :] = zero

        def finish_diag(i, _):
            for d in range(5):
                weight = 1.0 if 0 < d < 4 else 0.5
                for c in range(8):
                    a = (c + d) % 8
                    entry = d_ref[d_at(g, i, max(a, c), min(a, c)), :]
                    w_ref[w_at(g, OFF_DIAG + i * 40 + d * 8 + c), :] = weight * entry
            return 0

        lax.fori_loop(0, NBLK, finish_diag, 0)
        bias = jnp.broadcast_to(jnp.log(weight_ref[...]), (8, 128)) - 0.5 * x_ref[x_at(g, 48), :] - constant
        coarse = bias.astype(jnp.bfloat16).astype(jnp.float32)
        w_ref[w_at(g, OFF_BIAS), :] = coarse
        w_ref[w_at(g, OFF_BIAS + 1), :] = bias - coarse
        for n in range(OFF_BIAS + 2, FEATS):
            w_ref[w_at(g, n), :] = zero
        return 0

    lax.fori_loop(0, 2, finish, 0)


def product_groups(e_ref):
    width = e_ref.shape[1]

    def block(i):
        return e_ref[i * 8 : i * 8 + 8, :]

    def row(i):
        return jnp.broadcast_to(e_ref[i : i + 1, :], (8, width))

    groups = []
    for i in range(NBLK):
        for j in range(i):
            groups += [lambda i=i, j=j, a=a: row(i * 8 + a) * block(j) for a in range(8)]
    groups += [lambda j=j: row(48) * block(j) for j in range(NBLK)]
    groups += [lambda: row(48) * row(48)]
    for i in range(NBLK):
        for d in range(5):
            groups += [lambda i=i, d=d: block(i) * (pltpu.roll(block(i), 8 - d, 0) if d else block(i))]
    groups += [lambda: jnp.ones((8, width), jnp.float32)]
    groups += [lambda: jnp.zeros((8, width), jnp.float32)] * 2
    return groups


def prepare(se_ref, index_ref, root_ref, grid_ref, base_ref, level_ref, covar_ref, se2_ref, cov_ref, rows_ref):
    units = root_ref.shape[1]
    span = 128 // units
    comps = base_ref.shape[1]
    cov_ref[R * units :, :] = jnp.zeros((cov_ref.shape[0] - R * units, 128), jnp.float32)
    for u in range(units):
        root = root_ref[:, u, :]
        cov_ref[pl.ds(u, R, stride=units), 0:R] = lax.dot_general(
            root, root, (((1,), (1,)), ((), ())), precision=HIGHEST, preferred_element_type=jnp.float32
        )
    line = lax.broadcasted_iota(jnp.int32, (128, comps), 0)
    scale = jnp.zeros((1, comps), jnp.float32)
    for n in range(grid_ref.shape[0]):
        scale = jnp.where(level_ref[...] == n, grid_ref[n], scale)
    scale2 = scale * scale
    pick = jnp.concatenate(
        [(line == base_ref[...] + n * units).astype(jnp.float32) for n in range(span)], axis=1
    ).astype(jnp.bfloat16)
    blocks = cov_ref.shape[0] // 128
    rest = jnp.concatenate([cov_ref[n * 128 : n * 128 + 128, :].T[0:56] for n in range(blocks)], axis=0)
    total = None
    for _ in range(3):
        head = rest.astype(jnp.bfloat16)
        term = jnp.dot(head, pick, preferred_element_type=jnp.float32)
        total = term if total is None else total + term
        rest = rest - head.astype(jnp.float32)
    for i in range(R):
        block, n = divmod(i, span)
        covar_ref[i] = total[block * 56 : block * 56 + 56, n * 128 : n * 128 + 128] * scale2
    for t in range(index_ref.shape[0]):
        rows_ref[t : t + 1, 0:R] = se_ref[pl.ds(index_ref[t], 1), :]
    squares = rows_ref[...] * rows_ref[...]
    for i in range(R):
        se2_ref[i] = jnp.broadcast_to(squares[:, i : i + 1], se2_ref.shape[1:])


def sweep_kernel(
    se_in, index_in, root_in, grid_in, base_in, level_in, weight_in, w_ref,
    se_ref, index_ref, root_ref, grid_ref, base_ref, level_ref, weight_ref, sems,
    covar_ref, se2_ref, cov_ref, rows_ref, d_ref, b_ref, c_ref, v_ref, x_ref,
):
    sources = (se_in, index_in, root_in, grid_in, base_in, level_in, weight_in)
    places = (se_ref, index_ref, root_ref, grid_ref, base_ref, level_ref, weight_ref)
    copies = [pltpu.make_async_copy(a, b, sems.at[n]) for n, (a, b) in enumerate(zip(sources, places))]
    for copy in copies:
        copy.start()
    for copy in copies:
        copy.wait()
    prepare(se_ref, index_ref, root_ref, grid_ref, base_ref, level_ref, covar_ref, se2_ref, cov_ref, rows_ref)
    invert_all(covar_ref, se2_ref, weight_ref, w_ref, d_ref, b_ref, c_ref, v_ref, x_ref)


def sweep_stage(se_table, se_index, base_root, grid_scale, comp_base, comp_grid, weights):
    tissues = se_table.shape[1]
    units = base_root.shape[0]
    tiles = se_index.shape[0]
    comps = comp_base.shape[0]
    panel = pltpu.VMEM((2 * NBLK * 64 * 8, 128), jnp.float32)
    operands = (
        se_table, se_index, base_root.transpose(1, 0, 2), grid_scale,
        comp_base.reshape(1, comps), comp_grid.reshape(1, comps), weights.reshape(1, comps),
    )
    return pl.pallas_call(
        sweep_kernel,
        in_specs=[pl.BlockSpec(memory_space=pltpu.HBM)] * 7,
        out_specs=pl.BlockSpec(memory_space=pltpu.VMEM),
        out_shape=pltpu.VMEM((2 * FEATS * 8, 128), jnp.float32),
        scratch_shapes=[
            pltpu.VMEM(se_table.shape, jnp.float32),
            pltpu.SMEM((tiles,), jnp.int32),
            pltpu.VMEM((tissues, units, tissues), jnp.float32),
            pltpu.SMEM(grid_scale.shape, jnp.float32),
            pltpu.VMEM((1, comps), jnp.int32),
            pltpu.VMEM((1, comps), jnp.int32),
            pltpu.VMEM((1, comps), jnp.float32),
            pltpu.SemaphoreType.DMA((7,)),
            pltpu.VMEM((R, 56, comps), jnp.float32),
            pltpu.VMEM((R, tiles, comps), jnp.float32),
            pltpu.VMEM((-(-R * units // 128) * 128, 128), jnp.float32),
            pltpu.VMEM((tiles, 128), jnp.float32),
            panel,
            panel,
            panel,
            pltpu.VMEM((2 * 64 * 8, 128), jnp.float32),
            pltpu.VMEM((2 * 72 * 8, 128), jnp.float32),
        ],
        compiler_params=pltpu.CompilerParams(vmem_limit_bytes=32 * 1024 * 1024),
        cost_estimate=pl.CostEstimate(flops=250_000_000, bytes_accessed=60_000_000, transcendentals=0),
        name="sweep",
    )(*(pltpu.with_memory_space_constraint(operand, pltpu.HBM) for operand in operands))


def build_chunk(t, chunk, e_ref, w_ref, hi_ref, lo_ref, left_ref):
    first = (t // 8) * (FEATS * 8) + t % 8
    for n in (2 * chunk, 2 * chunk + 1):
        part = w_ref[pl.ds(first + n * 1024, 128, stride=8), :].T
        head = part.astype(jnp.bfloat16)
        left_ref[0:128, n * 128 : (n + 1) * 128] = head
        left_ref[128:256, n * 128 : (n + 1) * 128] = (part - head.astype(jnp.float32)).astype(jnp.bfloat16)
    groups = product_groups(e_ref.at[:, pl.ds(pl.multiple_of(t * TILE, TILE), TILE)])
    for n in range(chunk * 32, chunk * 32 + 32, 2):
        both = jnp.concatenate([groups[n](), groups[n + 1]()], axis=0)
        head = both.astype(jnp.bfloat16)
        rest = (both - head.astype(jnp.float32)).astype(jnp.bfloat16)
        hi_ref[n * 8 : n * 8 + 16, :] = head
        lo_ref[n * 8 : n * 8 + 16, :] = rest


def score_and_build(t, now, later, following, e_ref, w_ref, scores_ref, stats_ref):
    hi_ref, lo_ref, left_ref = now
    scores = None
    for chunk in range(FEATS // 256):
        rows = slice(chunk * 256, chunk * 256 + 256)
        main = jnp.dot(left_ref[:, rows], hi_ref[rows, :], preferred_element_type=jnp.float32)
        rest = jnp.dot(left_ref[0:128, rows], lo_ref[rows, :], preferred_element_type=jnp.float32)
        part = main[0:128] + (main[128:256] + rest)
        scores = part if scores is None else scores + part
        build_chunk(later, chunk, e_ref, w_ref, *following)
    cols = pl.ds(pl.multiple_of(t * TILE, TILE), TILE)
    top = jnp.max(scores, axis=0, keepdims=True)
    scores_ref[:, cols] = scores
    stats_ref[0:1, cols] = top
    stats_ref[1:2, cols] = jnp.sum(jnp.exp(scores - top), axis=0, keepdims=True)


def tile_kernel(
    count, all_pairs, all_comps, e_ref, w_ref, resp_ref, loglik_ref, logw_ref,
    hi_a, lo_a, left_a, hi_b, lo_b, left_b, scores_ref, stats_ref,
    other_ref, mine_ref, slots_ref, pair_sems, mass_sems,
):
    chip, core = lax.axis_index("pairs"), lax.axis_index("comp")
    mesh_id = pl.DeviceIdType.MESH
    barrier = pltpu.get_barrier_semaphore()
    pl.semaphore_signal(barrier, inc=1, device_id=(chip, 1 - core), device_id_type=mesh_id)

    def greet(d, _):
        pl.semaphore_signal(barrier, inc=1, device_id=((chip + d) % count, core), device_id_type=mesh_id)
        return 0

    lax.fori_loop(1, count, greet, 0)
    tiles = e_ref.shape[1] // TILE
    one, two = (hi_a, lo_a, left_a), (hi_b, lo_b, left_b)
    for chunk in range(FEATS // 256):
        build_chunk(0, chunk, e_ref, w_ref, *one)

    def two_tiles(s, _):
        score_and_build(2 * s, one, 2 * s + 1, two, e_ref, w_ref, scores_ref, stats_ref)
        score_and_build(2 * s + 1, two, (2 * s + 2) % tiles, one, e_ref, w_ref, scores_ref, stats_ref)
        return 0

    width = e_ref.shape[1] // 2

    def swap(h):
        cols = pl.ds(pl.multiple_of(h * width, width), width)
        return pltpu.make_async_remote_copy(
            src_ref=stats_ref.at[:, cols], dst_ref=other_ref.at[:, cols],
            send_sem=pair_sems.at[0, h], recv_sem=pair_sems.at[1, h],
            device_id=(chip, 1 - core), device_id_type=mesh_id,
        )

    def half(h, _):
        lax.fori_loop(0, tiles // 4, lambda s, z: two_tiles(h * (tiles // 4) + s, z), 0)

        @pl.when(h == 0)
        def _():
            pl.semaphore_wait(barrier, count)

        swap(h).start()
        return 0

    lax.fori_loop(0, 2, half, 0)

    def one_part(n, mass):
        cols = pl.ds(pl.multiple_of(n * TILE, TILE), TILE)
        m0, m1 = stats_ref[0:1, cols], other_ref[0:1, cols]
        top = jnp.maximum(m0, m1)
        total = stats_ref[1:2, cols] * jnp.exp(m0 - top) + other_ref[1:2, cols] * jnp.exp(m1 - top)
        loglik = top + jnp.log(total)
        loglik_ref[0:1, cols] = loglik
        resp = jnp.exp(scores_ref[:, cols] - loglik)
        resp_ref[:, cols] = resp
        for j in range(TILE // 128):
            mass = mass + resp[:, j * 128 : (j + 1) * 128]
        return mass

    def half_parts(h, mass):
        swap(h).wait()
        return lax.fori_loop(h * (tiles // 2), (h + 1) * (tiles // 2), one_part, mass)

    mass = lax.fori_loop(0, 2, half_parts, jnp.zeros((128, 128), jnp.float32))
    own = jnp.sum(mass.T, axis=0, keepdims=True)
    mine_ref[...] = own
    slots_ref[chip] = own

    def send(n, _):
        far = 1 + (n + (2 * count) // 3 - 1) % (count - 1)
        pltpu.make_async_remote_copy(
            src_ref=mine_ref, dst_ref=slots_ref.at[chip], send_sem=mass_sems.at[0], recv_sem=mass_sems.at[1],
            device_id=((chip + far) % count, core), device_id_type=mesh_id,
        ).start()
        return 0

    lax.fori_loop(0, count - 1, send, 0)
    every = pltpu.make_async_remote_copy(
        src_ref=slots_ref.at[pl.ds(0, count - 1)], dst_ref=slots_ref.at[pl.ds(0, count - 1)],
        send_sem=mass_sems.at[0], recv_sem=mass_sems.at[1],
        device_id=((chip + 1) % count, core), device_id_type=mesh_id,
    )
    every.wait_recv()
    parts = [slots_ref[n] for n in range(count)]
    while len(parts) > 1:
        parts = [parts[n] + parts[n + 1] for n in range(0, len(parts), 2)]
    logw_ref[...] = jnp.log((parts[0] + 1.0) / (all_pairs + all_comps))
    every.wait_send()


def write_kernel(resp_ref, loglik_ref, logw_ref, resp_out, loglik_out, logw_out, sems):
    pairs = ((resp_ref, resp_out), (loglik_ref, loglik_out), (logw_ref, logw_out))
    copies = [pltpu.make_async_copy(a, b, sems.at[n]) for n, (a, b) in enumerate(pairs)]
    for copy in copies:
        copy.start()
    for copy in copies:
        copy.wait()


def per_device(effects, se_table, se_index, base_root, grid_scale, comp_base, comp_grid, weights):
    pairs = effects.shape[1]
    comps = comp_base.shape[0]
    w = sweep_stage(se_table, se_index, base_root, grid_scale, comp_base, comp_grid, weights)
    count = lax.axis_size("pairs")
    vmem = pl.BlockSpec(memory_space=pltpu.VMEM)
    products = [
        pltpu.VMEM((FEATS, TILE), jnp.bfloat16),
        pltpu.VMEM((FEATS, TILE), jnp.bfloat16),
        pltpu.VMEM((256, FEATS), jnp.bfloat16),
    ]
    shapes = ((comps, pairs), (1, pairs), (1, comps))
    results = pl.pallas_call(
        functools.partial(tile_kernel, count, pairs * count, comps * lax.axis_size("comp")),
        in_specs=[vmem, vmem],
        out_specs=[vmem, vmem, vmem],
        out_shape=[pltpu.VMEM(shape, jnp.float32) for shape in shapes],
        scratch_shapes=products + products + [
            pltpu.VMEM((comps, pairs), jnp.float32),
            pltpu.VMEM((2, pairs), jnp.float32),
            pltpu.VMEM((2, pairs), jnp.float32),
            pltpu.VMEM((1, comps), jnp.float32),
            pltpu.VMEM((count, 1, comps), jnp.float32),
            pltpu.SemaphoreType.DMA((2, 2)),
            pltpu.SemaphoreType.DMA((2,)),
        ],
        compiler_params=pltpu.CompilerParams(
            collective_id=0, has_side_effects=True, vmem_limit_bytes=24 * 1024 * 1024,
        ),
        name="tiles",
    )(effects, w)
    resp, loglik, logw = pl.pallas_call(
        write_kernel,
        in_specs=[vmem, vmem, vmem],
        out_specs=[pl.BlockSpec(memory_space=pltpu.HBM)] * 3,
        out_shape=[jax.ShapeDtypeStruct(shape, jnp.float32) for shape in shapes],
        scratch_shapes=[pltpu.SemaphoreType.DMA((3,))],
        compiler_params=pltpu.CompilerParams(vmem_limit_bytes=4 * 1024 * 1024),
        name="write",
    )(*results)
    return (resp, logw.reshape(comps), loglik.reshape(pairs))


def solution(mesh):
    placed = (P(None, "pairs"), P(), P("pairs"), P(), P(), P("comp"), P("comp"), P("comp"))
    return jax.shard_map(
        per_device,
        mesh=mesh,
        in_specs=placed,
        out_specs=(P("comp", "pairs"), P("comp"), P("pairs")),
        check_vma=False,
    )
```

```python
import functools
import math

import jax
import jax.numpy as jnp
from jax import lax
from jax.experimental import pallas as pl
from jax.experimental.pallas import tpu as pltpu
from jax.sharding import PartitionSpec as P

TILE = 512
R = 49
NBLK = 6
FEATS = 1280
OFF_BORDER = 960
OFF_LAST = 1008
OFF_DIAG = 1016
OFF_BIAS = 1256
HIGHEST = lax.Precision.HIGHEST


def row8(index):
    return pl.ds(pl.multiple_of(index * 8, 8), 8)


def invert_all(covar_ref, se2_ref, weight_ref, w_ref, d_ref, b_ref, c_ref, v_ref, x_ref):
    def w_at(g, f):
        return row8(g * FEATS + f)

    def d_at(g, block, a, c):
        return row8((g * NBLK + block) * 64 + a * 8 + c)

    def p_at(g, block, a, c):
        return row8((g * NBLK + block) * 64 + a * 8 + c)

    def pair_base(i, j):
        return (i * (i - 1) // 2 + j) * 64

    def cov(i, j):
        return jnp.broadcast_to(covar_ref[i, pl.ds(j, 1), :], (8, 128))

    def x_at(g, n):
        return row8(g * 72 + n)

    for g in range(2):
        se_last = se2_ref[48, g * 8 : g * 8 + 8, :]
        pivot = cov(48, 48) + se_last
        inv = 1.0 / pivot
        x_ref[x_at(g, 48), :] = jnp.log(pivot)
        w_ref[w_at(g, OFF_LAST), :] = -inv
        for i in range(48):
            edge = cov(48, i)
            x_ref[x_at(g, i), :] = edge
            w_ref[w_at(g, OFF_BORDER + i), :] = edge * inv

    def init_group(g, _):
        def init_row(i, _):
            edges = [x_ref[x_at(g, i * 8 + a), :] for a in range(8)]

            def init_pair(j, _):
                scaled = [w_ref[w_at(g, OFF_BORDER + j * 8 + c), :] for c in range(8)]
                base = pair_base(i, j)
                for a in range(8):
                    for c in range(8):
                        w_ref[w_at(g, base + a * 8 + c), :] = cov(i * 8 + a, j * 8 + c) - edges[a] * scaled[c]
                return 0

            lax.fori_loop(0, i, init_pair, 0)
            scaled = [w_ref[w_at(g, OFF_BORDER + i * 8 + c), :] for c in range(8)]
            for a in range(8):
                for c in range(a + 1):
                    entry = cov(i * 8 + a, i * 8 + c) - edges[a] * scaled[c]
                    if a == c:
                        entry = entry + se2_ref[i * 8 + a, pl.ds(pl.multiple_of(g * 8, 8), 8), :]
                    d_ref[d_at(g, i, a, c), :] = entry
            return 0

        lax.fori_loop(0, NBLK, init_row, 0)
        return 0

    lax.fori_loop(0, 2, init_group, 0)

    def pivot_block(k):
        for g in range(2):
            m = {(a, c): d_ref[d_at(g, k, a, c), :] for a in range(8) for c in range(a + 1)}
            product = None
            for s in range(8):
                p = m[s, s]
                product = p if product is None else product * p
                inv = 1.0 / p
                col = {a: (m[a, s] if a > s else m[s, a]) for a in range(8) if a != s}
                scaled = {a: col[a] * inv for a in col}
                for a in col:
                    for c in col:
                        if c <= a:
                            m[a, c] = m[a, c] - scaled[a] * col[c]
                for a in col:
                    m[max(a, s), min(a, s)] = scaled[a]
                m[s, s] = -inv
            x_ref[x_at(g, 48), :] = x_ref[x_at(g, 48), :] + jnp.log(product)
            for a in range(8):
                for c in range(8):
                    entry = m[max(a, c), min(a, c)]
                    if c <= a:
                        d_ref[d_at(g, k, a, c), :] = entry
                    v_ref[row8(g * 64 + a * 8 + c), :] = -entry

    def scale_block(g, k, j, swap):
        base = pair_base(k, j) if swap else pair_base(j, k)
        for half in range(4):
            rows = range(half // 2 * 4, half // 2 * 4 + 4)
            cols = range(half % 2 * 4, half % 2 * 4 + 4)
            acc = {}
            for l in range(8):
                left = {}
                for a in rows:
                    if half % 2:
                        left[a] = c_ref[p_at(g, j, a, l), :]
                    else:
                        left[a] = w_ref[w_at(g, base + (l * 8 + a if swap else a * 8 + l)), :]
                        c_ref[p_at(g, j, a, l), :] = left[a]
                for c in cols:
                    right = v_ref[row8(g * 64 + l * 8 + c), :]
                    for a in rows:
                        term = left[a] * right
                        acc[a, c] = term if l == 0 else acc[a, c] + term
            for a in rows:
                for c in cols:
                    b_ref[p_at(g, j, a, c), :] = acc[a, c]
        for a in range(8):
            for c in range(8):
                w_ref[w_at(g, base + (c * 8 + a if swap else a * 8 + c)), :] = b_ref[p_at(g, j, a, c), :]

    def scale_border(g, k):
        old = [w_ref[w_at(g, OFF_BORDER + k * 8 + m), :] for m in range(8)]
        total = w_ref[w_at(g, OFF_LAST), :]
        for c in range(8):
            new = old[0] * v_ref[row8(g * 64 + c), :]
            for l in range(1, 8):
                new = new + old[l] * v_ref[row8(g * 64 + l * 8 + c), :]
            x_ref[x_at(g, 49 + c), :] = new
            w_ref[w_at(g, OFF_BORDER + k * 8 + c), :] = new
            total = total - new * old[c]
        w_ref[w_at(g, OFF_LAST), :] = total

    def update_pair(g, i, j):
        base = pair_base(i, j)
        for half in range(4):
            rows = range(half // 2 * 4, half // 2 * 4 + 4)
            cols = range(half % 2 * 4, half % 2 * 4 + 4)
            acc = {(a, c): w_ref[w_at(g, base + a * 8 + c), :] for a in rows for c in cols}
            for m in range(8):
                left = {a: b_ref[p_at(g, i, a, m), :] for a in rows}
                for c in cols:
                    right = c_ref[p_at(g, j, c, m), :]
                    for a in rows:
                        acc[a, c] = acc[a, c] - left[a] * right
            for a in rows:
                for c in cols:
                    w_ref[w_at(g, base + a * 8 + c), :] = acc[a, c]

    def update_diag(g, i):
        for rows in (range(0, 6), range(6, 8)):
            acc = {(a, c): d_ref[d_at(g, i, a, c), :] for a in rows for c in range(a + 1)}
            if rows[0]:
                edge = [w_ref[w_at(g, OFF_BORDER + i * 8 + c), :] for c in range(8)]
            for m in range(8):
                left = {a: b_ref[p_at(g, i, a, m), :] for a in rows}
                if rows[0]:
                    last = x_ref[x_at(g, 49 + m), :]
                for c in range(rows[-1] + 1):
                    right = c_ref[p_at(g, i, c, m), :]
                    for a in rows:
                        if c <= a:
                            acc[a, c] = acc[a, c] - left[a] * right
                    if rows[0]:
                        edge[c] = edge[c] - last * right
            for a, c in acc:
                d_ref[d_at(g, i, a, c), :] = acc[a, c]
            if rows[0]:
                for c in range(8):
                    w_ref[w_at(g, OFF_BORDER + i * 8 + c), :] = edge[c]

    def sweep(k, _):
        pivot_block(k)

        def scale_one(j, swap):
            for g in range(2):
                scale_block(g, k, j, swap)

        lax.fori_loop(0, k, lambda j, z: (scale_one(j, True), z)[1], 0)
        lax.fori_loop(k + 1, NBLK, lambda j, z: (scale_one(j, False), z)[1], 0)
        for g in range(2):
            scale_border(g, k)

        def update_row(t, _):
            i = t + (t >= k).astype(jnp.int32)

            def update_one(s, _):
                for g in range(2):
                    update_pair(g, i, s + (s >= k).astype(jnp.int32))
                return 0

            lax.fori_loop(0, t, update_one, 0)
            for g in range(2):
                update_diag(g, i)
            return 0

        lax.fori_loop(0, NBLK - 1, update_row, 0)
        return 0

    lax.fori_loop(0, NBLK, sweep, 0)

    zero = jnp.zeros((8, 128), jnp.float32)
    constant = 0.5 * R * math.log(2.0 * math.pi)

    def finish(g, _):
        w_ref[w_at(g, OFF_LAST), :] = 0.5 * w_ref[w_at(g, OFF_LAST), :]
        for n in range(1, 8):
            w_ref[w_at(g, OFF_LAST + n), :] = zero

        def finish_diag(i, _):
            for d in range(5):
                weight = 1.0 if 0 < d < 4 else 0.5
                for c in range(8):
                    a = (c + d) % 8
                    entry = d_ref[d_at(g, i, max(a, c), min(a, c)), :]
                    w_ref[w_at(g, OFF_DIAG + i * 40 + d * 8 + c), :] = weight * entry
            return 0

        lax.fori_loop(0, NBLK, finish_diag, 0)
        bias = jnp.broadcast_to(jnp.log(weight_ref[...]), (8, 128)) - 0.5 * x_ref[x_at(g, 48), :] - constant
        coarse = bias.astype(jnp.bfloat16).astype(jnp.float32)
        w_ref[w_at(g, OFF_BIAS), :] = coarse
        w_ref[w_at(g, OFF_BIAS + 1), :] = bias - coarse
        for n in range(OFF_BIAS + 2, FEATS):
            w_ref[w_at(g, n), :] = zero
        return 0

    lax.fori_loop(0, 2, finish, 0)


def product_groups(e_ref):
    width = e_ref.shape[1]

    def block(i):
        return e_ref[i * 8 : i * 8 + 8, :]

    def row(i):
        return jnp.broadcast_to(e_ref[i : i + 1, :], (8, width))

    groups = []
    for i in range(NBLK):
        for j in range(i):
            groups += [lambda i=i, j=j, a=a: row(i * 8 + a) * block(j) for a in range(8)]
    groups += [lambda j=j: row(48) * block(j) for j in range(NBLK)]
    groups += [lambda: row(48) * row(48)]
    for i in range(NBLK):
        for d in range(5):
            groups += [lambda i=i, d=d: block(i) * (pltpu.roll(block(i), 8 - d, 0) if d else block(i))]
    groups += [lambda: jnp.ones((8, width), jnp.float32)]
    groups += [lambda: jnp.zeros((8, width), jnp.float32)] * 2
    return groups


def prepare_errors(se_ref, index_ref, se2_ref, rows_ref):
    for t in range(index_ref.shape[0]):
        rows_ref[t : t + 1, 0:R] = se_ref[pl.ds(index_ref[t], 1), :]
    squares = rows_ref[...] * rows_ref[...]
    for i in range(R):
        se2_ref[i] = jnp.broadcast_to(squares[:, i : i + 1], se2_ref.shape[1:])


def prepare(root_ref, grid_ref, base_ref, level_ref, covar_ref, cov_ref):
    units = root_ref.shape[1]
    span = 128 // units
    comps = base_ref.shape[1]
    cov_ref[R * units :, :] = jnp.zeros((cov_ref.shape[0] - R * units, 128), jnp.float32)
    for u in range(units):
        root = root_ref[:, u, :]
        cov_ref[pl.ds(u, R, stride=units), 0:R] = lax.dot_general(
            root, root, (((1,), (1,)), ((), ())), precision=HIGHEST, preferred_element_type=jnp.float32
        )
    line = lax.broadcasted_iota(jnp.int32, (128, comps), 0)
    scale = jnp.zeros((1, comps), jnp.float32)
    for n in range(grid_ref.shape[0]):
        scale = jnp.where(level_ref[...] == n, grid_ref[n], scale)
    scale2 = scale * scale
    pick = jnp.concatenate(
        [(line == base_ref[...] + n * units).astype(jnp.float32) for n in range(span)], axis=1
    ).astype(jnp.bfloat16)
    blocks = cov_ref.shape[0] // 128
    rest = jnp.concatenate([cov_ref[n * 128 : n * 128 + 128, :].T[0:56] for n in range(blocks)], axis=0)
    total = None
    for _ in range(3):
        head = rest.astype(jnp.bfloat16)
        term = jnp.dot(head, pick, preferred_element_type=jnp.float32)
        total = term if total is None else total + term
        rest = rest - head.astype(jnp.float32)
    for i in range(R):
        block, n = divmod(i, span)
        covar_ref[i] = total[block * 56 : block * 56 + 56, n * 128 : n * 128 + 128] * scale2


def sweep_kernel(
    se_in, index_in, root_in, grid_in, base_in, level_in, weight_in, w_ref,
    se_ref, index_ref, root_ref, grid_ref, base_ref, level_ref, weight_ref, sems,
    covar_ref, se2_ref, cov_ref, rows_ref, d_ref, b_ref, c_ref, v_ref, x_ref,
):
    sources = (se_in, index_in, root_in, grid_in, base_in, level_in, weight_in)
    places = (se_ref, index_ref, root_ref, grid_ref, base_ref, level_ref, weight_ref)
    copies = [pltpu.make_async_copy(a, b, sems.at[n]) for n, (a, b) in enumerate(zip(sources, places))]
    for copy in copies:
        copy.start()
    for n in (0, 1, 3, 4, 5, 6):
        copies[n].wait()
    prepare_errors(se_ref, index_ref, se2_ref, rows_ref)
    copies[2].wait()
    prepare(root_ref, grid_ref, base_ref, level_ref, covar_ref, cov_ref)
    invert_all(covar_ref, se2_ref, weight_ref, w_ref, d_ref, b_ref, c_ref, v_ref, x_ref)


def sweep_stage(se_table, se_index, base_root, grid_scale, comp_base, comp_grid, weights):
    tissues = se_table.shape[1]
    units = base_root.shape[0]
    tiles = se_index.shape[0]
    comps = comp_base.shape[0]
    panel = pltpu.VMEM((2 * NBLK * 64 * 8, 128), jnp.float32)
    operands = (
        se_table, se_index, base_root.transpose(1, 0, 2), grid_scale,
        comp_base.reshape(1, comps), comp_grid.reshape(1, comps), weights.reshape(1, comps),
    )
    return pl.pallas_call(
        sweep_kernel,
        in_specs=[pl.BlockSpec(memory_space=pltpu.HBM)] * 7,
        out_specs=pl.BlockSpec(memory_space=pltpu.VMEM),
        out_shape=pltpu.VMEM((2 * FEATS * 8, 128), jnp.float32),
        scratch_shapes=[
            pltpu.VMEM(se_table.shape, jnp.float32),
            pltpu.SMEM((tiles,), jnp.int32),
            pltpu.VMEM((tissues, units, tissues), jnp.float32),
            pltpu.SMEM(grid_scale.shape, jnp.float32),
            pltpu.VMEM((1, comps), jnp.int32),
            pltpu.VMEM((1, comps), jnp.int32),
            pltpu.VMEM((1, comps), jnp.float32),
            pltpu.SemaphoreType.DMA((7,)),
            pltpu.VMEM((R, 56, comps), jnp.float32),
            pltpu.VMEM((R, tiles, comps), jnp.float32),
            pltpu.VMEM((-(-R * units // 128) * 128, 128), jnp.float32),
            pltpu.VMEM((tiles, 128), jnp.float32),
            panel,
            panel,
            panel,
            pltpu.VMEM((2 * 64 * 8, 128), jnp.float32),
            pltpu.VMEM((2 * 72 * 8, 128), jnp.float32),
        ],
        compiler_params=pltpu.CompilerParams(vmem_limit_bytes=32 * 1024 * 1024),
        cost_estimate=pl.CostEstimate(flops=250_000_000, bytes_accessed=60_000_000, transcendentals=0),
        name="sweep",
    )(*(pltpu.with_memory_space_constraint(operand, pltpu.HBM) for operand in operands))


def build_chunk(t, chunk, e_ref, w_ref, hi_ref, lo_ref, left_ref):
    first = (t // 8) * (FEATS * 8) + t % 8
    for n in (2 * chunk, 2 * chunk + 1):
        part = w_ref[pl.ds(first + n * 1024, 128, stride=8), :].T
        head = part.astype(jnp.bfloat16)
        left_ref[0:128, n * 128 : (n + 1) * 128] = head
        left_ref[128:256, n * 128 : (n + 1) * 128] = (part - head.astype(jnp.float32)).astype(jnp.bfloat16)
    groups = product_groups(e_ref.at[:, pl.ds(pl.multiple_of(t * TILE, TILE), TILE)])
    for n in range(chunk * 32, chunk * 32 + 32, 2):
        both = jnp.concatenate([groups[n](), groups[n + 1]()], axis=0)
        head = both.astype(jnp.bfloat16)
        rest = (both - head.astype(jnp.float32)).astype(jnp.bfloat16)
        hi_ref[n * 8 : n * 8 + 16, :] = head
        lo_ref[n * 8 : n * 8 + 16, :] = rest


def score_and_build(t, now, later, following, e_ref, w_ref, scores_ref, stats_ref):
    hi_ref, lo_ref, left_ref = now
    scores = None
    for chunk in range(FEATS // 256):
        rows = slice(chunk * 256, chunk * 256 + 256)
        main = jnp.dot(left_ref[:, rows], hi_ref[rows, :], preferred_element_type=jnp.float32)
        rest = jnp.dot(left_ref[0:128, rows], lo_ref[rows, :], preferred_element_type=jnp.float32)
        part = main[0:128] + (main[128:256] + rest)
        scores = part if scores is None else scores + part
        build_chunk(later, chunk, e_ref, w_ref, *following)
    cols = pl.ds(pl.multiple_of(t * TILE, TILE), TILE)
    top = jnp.max(scores, axis=0, keepdims=True)
    scores_ref[:, cols] = scores
    stats_ref[0:1, cols] = top
    stats_ref[1:2, cols] = jnp.sum(jnp.exp(scores - top), axis=0, keepdims=True)


def tile_kernel(
    count, all_pairs, all_comps, e_ref, w_ref, resp_ref, loglik_ref, logw_ref,
    hi_a, lo_a, left_a, hi_b, lo_b, left_b, scores_ref, stats_ref,
    other_ref, mine_ref, slots_ref, pair_sems, mass_sems,
):
    chip, core = lax.axis_index("pairs"), lax.axis_index("comp")
    mesh_id = pl.DeviceIdType.MESH
    barrier = pltpu.get_barrier_semaphore()
    pl.semaphore_signal(barrier, inc=1, device_id=(chip, 1 - core), device_id_type=mesh_id)

    def greet(peer, _):
        pl.semaphore_signal(barrier, inc=1, device_id=(peer, core), device_id_type=mesh_id)
        return 0

    lax.fori_loop(0, chip, greet, 0)
    lax.fori_loop(chip + 1, count, greet, 0)
    tiles = e_ref.shape[1] // TILE
    one, two = (hi_a, lo_a, left_a), (hi_b, lo_b, left_b)
    for chunk in range(FEATS // 256):
        build_chunk(0, chunk, e_ref, w_ref, *one)

    def two_tiles(s, _):
        score_and_build(2 * s, one, 2 * s + 1, two, e_ref, w_ref, scores_ref, stats_ref)
        score_and_build(2 * s + 1, two, (2 * s + 2) % tiles, one, e_ref, w_ref, scores_ref, stats_ref)
        return 0

    width = e_ref.shape[1] // 2

    def swap(h):
        cols = pl.ds(pl.multiple_of(h * width, width), width)
        return pltpu.make_async_remote_copy(
            src_ref=stats_ref.at[:, cols], dst_ref=other_ref.at[:, cols],
            send_sem=pair_sems.at[0, h], recv_sem=pair_sems.at[1, h],
            device_id=(chip, 1 - core), device_id_type=mesh_id,
        )

    def half(h, _):
        lax.fori_loop(0, tiles // 4, lambda s, z: two_tiles(h * (tiles // 4) + s, z), 0)

        @pl.when(h == 0)
        def _():
            pl.semaphore_wait(barrier, count)

        swap(h).start()
        return 0

    lax.fori_loop(0, 2, half, 0)

    def one_part(n, mass):
        cols = pl.ds(pl.multiple_of(n * TILE, TILE), TILE)
        m0, m1 = stats_ref[0:1, cols], other_ref[0:1, cols]
        top = jnp.maximum(m0, m1)
        total = stats_ref[1:2, cols] * jnp.exp(m0 - top) + other_ref[1:2, cols] * jnp.exp(m1 - top)
        loglik = top + jnp.log(total)
        loglik_ref[0:1, cols] = loglik
        resp = jnp.exp(scores_ref[:, cols] - loglik)
        resp_ref[:, cols] = resp
        for j in range(TILE // 128):
            mass = mass + resp[:, j * 128 : (j + 1) * 128]
        return mass

    def two_parts(n, mass):
        return one_part(2 * n + 1, one_part(2 * n, mass))

    def half_parts(h, mass):
        swap(h).wait()
        return lax.fori_loop(h * (tiles // 4), (h + 1) * (tiles // 4), two_parts, mass)

    mass = lax.fori_loop(0, 2, half_parts, jnp.zeros((128, 128), jnp.float32))
    own = jnp.sum(mass.T, axis=0, keepdims=True)
    mine_ref[...] = own
    slots_ref[chip] = own

    def send(n, _):
        far = 1 + (n + (2 * count) // 3 - 1) % (count - 1)
        pltpu.make_async_remote_copy(
            src_ref=mine_ref, dst_ref=slots_ref.at[chip], send_sem=mass_sems.at[0], recv_sem=mass_sems.at[1],
            device_id=((chip + far) % count, core), device_id_type=mesh_id,
        ).start()
        return 0

    lax.fori_loop(0, count - 1, send, 0)
    every = pltpu.make_async_remote_copy(
        src_ref=slots_ref.at[pl.ds(0, count - 1)], dst_ref=slots_ref.at[pl.ds(0, count - 1)],
        send_sem=mass_sems.at[0], recv_sem=mass_sems.at[1],
        device_id=((chip + 1) % count, core), device_id_type=mesh_id,
    )
    every.wait_recv()
    parts = [slots_ref[n] for n in range(count)]
    while len(parts) > 1:
        parts = [parts[n] + parts[n + 1] for n in range(0, len(parts), 2)]
    logw_ref[...] = jnp.log((parts[0] + 1.0) / (all_pairs + all_comps))
    every.wait_send()


def write_kernel(resp_ref, loglik_ref, logw_ref, resp_out, loglik_out, logw_out, sems):
    pairs = ((resp_ref, resp_out), (loglik_ref, loglik_out), (logw_ref, logw_out))
    copies = [pltpu.make_async_copy(a, b, sems.at[n]) for n, (a, b) in enumerate(pairs)]
    for copy in copies:
        copy.start()
    for copy in copies:
        copy.wait()


def per_device(effects, se_table, se_index, base_root, grid_scale, comp_base, comp_grid, weights):
    pairs = effects.shape[1]
    comps = comp_base.shape[0]
    w = sweep_stage(se_table, se_index, base_root, grid_scale, comp_base, comp_grid, weights)
    count = lax.axis_size("pairs")
    vmem = pl.BlockSpec(memory_space=pltpu.VMEM)
    products = [
        pltpu.VMEM((FEATS, TILE), jnp.bfloat16),
        pltpu.VMEM((FEATS, TILE), jnp.bfloat16),
        pltpu.VMEM((256, FEATS), jnp.bfloat16),
    ]
    shapes = ((comps, pairs), (1, pairs), (1, comps))
    results = pl.pallas_call(
        functools.partial(tile_kernel, count, pairs * count, comps * lax.axis_size("comp")),
        in_specs=[vmem, vmem],
        out_specs=[vmem, vmem, vmem],
        out_shape=[pltpu.VMEM(shape, jnp.float32) for shape in shapes],
        scratch_shapes=products + products + [
            pltpu.VMEM((comps, pairs), jnp.float32),
            pltpu.VMEM((2, pairs), jnp.float32),
            pltpu.VMEM((2, pairs), jnp.float32),
            pltpu.VMEM((1, comps), jnp.float32),
            pltpu.VMEM((count, 1, comps), jnp.float32),
            pltpu.SemaphoreType.DMA((2, 2)),
            pltpu.SemaphoreType.DMA((2,)),
        ],
        compiler_params=pltpu.CompilerParams(
            collective_id=0, has_side_effects=True, vmem_limit_bytes=24 * 1024 * 1024,
        ),
        name="tiles",
    )(effects, w)
    resp, loglik, logw = pl.pallas_call(
        write_kernel,
        in_specs=[vmem, vmem, vmem],
        out_specs=[pl.BlockSpec(memory_space=pltpu.HBM)] * 3,
        out_shape=[jax.ShapeDtypeStruct(shape, jnp.float32) for shape in shapes],
        scratch_shapes=[pltpu.SemaphoreType.DMA((3,))],
        compiler_params=pltpu.CompilerParams(vmem_limit_bytes=4 * 1024 * 1024),
        name="write",
    )(*results)
    return (resp, logw.reshape(comps), loglik.reshape(pairs))


def solution(mesh):
    placed = (P(None, "pairs"), P(), P("pairs"), P(), P(), P("comp"), P("comp"), P("comp"))
    return jax.shard_map(
        per_device,
        mesh=mesh,
        in_specs=placed,
        out_specs=(P("comp", "pairs"), P("comp"), P("pairs")),
        check_vma=False,
    )
```

```python
import functools
import math

import jax
import jax.numpy as jnp
from jax import lax
from jax.experimental import pallas as pl
from jax.experimental.pallas import tpu as pltpu
from jax.sharding import PartitionSpec as P

TILE = 512
R = 49
NBLK = 6
FEATS = 1280
OFF_BORDER = 960
OFF_LAST = 1008
OFF_DIAG = 1016
OFF_BIAS = 1256
HIGHEST = lax.Precision.HIGHEST


def row8(index):
    return pl.ds(pl.multiple_of(index * 8, 8), 8)


def invert_all(covar_ref, se2_ref, weight_ref, w_ref, d_ref, b_ref, c_ref, v_ref, x_ref):
    def w_at(g, f):
        return row8(g * FEATS + f)

    def d_at(g, block, a, c):
        return row8((g * NBLK + block) * 64 + a * 8 + c)

    def p_at(g, block, a, c):
        return row8((g * NBLK + block) * 64 + a * 8 + c)

    def pair_base(i, j):
        return (i * (i - 1) // 2 + j) * 64

    def cov(i, j):
        return jnp.broadcast_to(covar_ref[i, pl.ds(j, 1), :], (8, 128))

    def x_at(g, n):
        return row8(g * 72 + n)

    for g in range(2):
        se_last = se2_ref[48, g * 8 : g * 8 + 8, :]
        pivot = cov(48, 48) + se_last
        inv = 1.0 / pivot
        x_ref[x_at(g, 48), :] = jnp.log(pivot)
        w_ref[w_at(g, OFF_LAST), :] = -inv
        for i in range(48):
            edge = cov(48, i)
            x_ref[x_at(g, i), :] = edge
            w_ref[w_at(g, OFF_BORDER + i), :] = edge * inv

    def init_row(i, _):
        edges = {(g, a): x_ref[x_at(g, i * 8 + a), :] for g in range(2) for a in range(8)}

        def init_pair(j, _):
            scaled = {(g, c): w_ref[w_at(g, OFF_BORDER + j * 8 + c), :] for g in range(2) for c in range(8)}
            base = pair_base(i, j)
            for a in range(8):
                for c in range(8):
                    entry = cov(i * 8 + a, j * 8 + c)
                    for g in range(2):
                        w_ref[w_at(g, base + a * 8 + c), :] = entry - edges[g, a] * scaled[g, c]
            return 0

        lax.fori_loop(0, i, init_pair, 0)
        scaled = {(g, c): w_ref[w_at(g, OFF_BORDER + i * 8 + c), :] for g in range(2) for c in range(8)}
        for a in range(8):
            for c in range(a + 1):
                for g in range(2):
                    entry = cov(i * 8 + a, i * 8 + c) - edges[g, a] * scaled[g, c]
                    if a == c:
                        entry = entry + se2_ref[i * 8 + a, g * 8 : g * 8 + 8, :]
                    d_ref[d_at(g, i, a, c), :] = entry
        return 0

    lax.fori_loop(0, NBLK, init_row, 0)

    def pivot_block(k):
        for g in range(2):
            m = {(a, c): d_ref[d_at(g, k, a, c), :] for a in range(8) for c in range(a + 1)}
            product = None
            for s in range(8):
                p = m[s, s]
                product = p if product is None else product * p
                inv = 1.0 / p
                col = {a: (m[a, s] if a > s else m[s, a]) for a in range(8) if a != s}
                scaled = {a: col[a] * inv for a in col}
                for a in col:
                    for c in col:
                        if c <= a:
                            m[a, c] = m[a, c] - scaled[a] * col[c]
                for a in col:
                    m[max(a, s), min(a, s)] = scaled[a]
                m[s, s] = -inv
            x_ref[x_at(g, 48), :] = x_ref[x_at(g, 48), :] + jnp.log(product)
            for a in range(8):
                for c in range(8):
                    entry = m[max(a, c), min(a, c)]
                    if c <= a:
                        d_ref[d_at(g, k, a, c), :] = entry
                    v_ref[row8(g * 64 + a * 8 + c), :] = -entry

    def scale_block(g, k, j, swap):
        base = pair_base(k, j) if swap else pair_base(j, k)
        for half in range(4):
            rows = range(half // 2 * 4, half // 2 * 4 + 4)
            cols = range(half % 2 * 4, half % 2 * 4 + 4)
            acc = {}
            for l in range(8):
                left = {}
                for a in rows:
                    if half % 2:
                        left[a] = c_ref[p_at(g, j, a, l), :]
                    else:
                        left[a] = w_ref[w_at(g, base + (l * 8 + a if swap else a * 8 + l)), :]
                        c_ref[p_at(g, j, a, l), :] = left[a]
                for c in cols:
                    right = v_ref[row8(g * 64 + l * 8 + c), :]
                    for a in rows:
                        term = left[a] * right
                        acc[a, c] = term if l == 0 else acc[a, c] + term
            for a in rows:
                for c in cols:
                    b_ref[p_at(g, j, a, c), :] = acc[a, c]
        for a in range(8):
            for c in range(8):
                w_ref[w_at(g, base + (c * 8 + a if swap else a * 8 + c)), :] = b_ref[p_at(g, j, a, c), :]

    def scale_border(g, k):
        old = [w_ref[w_at(g, OFF_BORDER + k * 8 + m), :] for m in range(8)]
        total = w_ref[w_at(g, OFF_LAST), :]
        for c in range(8):
            new = old[0] * v_ref[row8(g * 64 + c), :]
            for l in range(1, 8):
                new = new + old[l] * v_ref[row8(g * 64 + l * 8 + c), :]
            x_ref[x_at(g, 49 + c), :] = new
            w_ref[w_at(g, OFF_BORDER + k * 8 + c), :] = new
            total = total - new * old[c]
        w_ref[w_at(g, OFF_LAST), :] = total

    def update_pair(g, i, j):
        base = pair_base(i, j)
        for half in range(4):
            rows = range(half // 2 * 4, half // 2 * 4 + 4)
            cols = range(half % 2 * 4, half % 2 * 4 + 4)
            acc = {(a, c): w_ref[w_at(g, base + a * 8 + c), :] for a in rows for c in cols}
            for m in range(8):
                left = {a: b_ref[p_at(g, i, a, m), :] for a in rows}
                for c in cols:
                    right = c_ref[p_at(g, j, c, m), :]
                    for a in rows:
                        acc[a, c] = acc[a, c] - left[a] * right
            for a in rows:
                for c in cols:
                    w_ref[w_at(g, base + a * 8 + c), :] = acc[a, c]

    def update_diag(g, i):
        for rows in (range(0, 6), range(6, 8)):
            acc = {(a, c): d_ref[d_at(g, i, a, c), :] for a in rows for c in range(a + 1)}
            if rows[0]:
                edge = [w_ref[w_at(g, OFF_BORDER + i * 8 + c), :] for c in range(8)]
            for m in range(8):
                left = {a: b_ref[p_at(g, i, a, m), :] for a in rows}
                if rows[0]:
                    last = x_ref[x_at(g, 49 + m), :]
                for c in range(rows[-1] + 1):
                    right = c_ref[p_at(g, i, c, m), :]
                    for a in rows:
                        if c <= a:
                            acc[a, c] = acc[a, c] - left[a] * right
                    if rows[0]:
                        edge[c] = edge[c] - last * right
            for a, c in acc:
                d_ref[d_at(g, i, a, c), :] = acc[a, c]
            if rows[0]:
                for c in range(8):
                    w_ref[w_at(g, OFF_BORDER + i * 8 + c), :] = edge[c]

    def sweep(k, _):
        pivot_block(k)

        def scale_one(j, swap):
            for g in range(2):
                scale_block(g, k, j, swap)

        lax.fori_loop(0, k, lambda j, z: (scale_one(j, True), z)[1], 0)
        lax.fori_loop(k + 1, NBLK, lambda j, z: (scale_one(j, False), z)[1], 0)
        for g in range(2):
            scale_border(g, k)

        def update_row(t, _):
            i = t + (t >= k).astype(jnp.int32)

            def update_one(s, _):
                for g in range(2):
                    update_pair(g, i, s + (s >= k).astype(jnp.int32))
                return 0

            lax.fori_loop(0, t, update_one, 0)
            for g in range(2):
                update_diag(g, i)
            return 0

        lax.fori_loop(0, NBLK - 1, update_row, 0)
        return 0

    lax.fori_loop(0, NBLK, sweep, 0)

    zero = jnp.zeros((8, 128), jnp.float32)
    constant = 0.5 * R * math.log(2.0 * math.pi)

    def finish(g, _):
        w_ref[w_at(g, OFF_LAST), :] = 0.5 * w_ref[w_at(g, OFF_LAST), :]
        for n in range(1, 8):
            w_ref[w_at(g, OFF_LAST + n), :] = zero

        def finish_diag(i, _):
            for d in range(5):
                weight = 1.0 if 0 < d < 4 else 0.5
                for c in range(8):
                    a = (c + d) % 8
                    entry = d_ref[d_at(g, i, max(a, c), min(a, c)), :]
                    w_ref[w_at(g, OFF_DIAG + i * 40 + d * 8 + c), :] = weight * entry
            return 0

        lax.fori_loop(0, NBLK, finish_diag, 0)
        bias = jnp.broadcast_to(jnp.log(weight_ref[...]), (8, 128)) - 0.5 * x_ref[x_at(g, 48), :] - constant
        coarse = bias.astype(jnp.bfloat16).astype(jnp.float32)
        w_ref[w_at(g, OFF_BIAS), :] = coarse
        w_ref[w_at(g, OFF_BIAS + 1), :] = bias - coarse
        for n in range(OFF_BIAS + 2, FEATS):
            w_ref[w_at(g, n), :] = zero
        return 0

    lax.fori_loop(0, 2, finish, 0)


def product_groups(e_ref):
    width = e_ref.shape[1]

    def block(i):
        return e_ref[i * 8 : i * 8 + 8, :]

    def row(i):
        return jnp.broadcast_to(e_ref[i : i + 1, :], (8, width))

    groups = []
    for i in range(NBLK):
        for j in range(i):
            groups += [lambda i=i, j=j, a=a: row(i * 8 + a) * block(j) for a in range(8)]
    groups += [lambda j=j: row(48) * block(j) for j in range(NBLK)]
    groups += [lambda: row(48) * row(48)]
    for i in range(NBLK):
        for d in range(5):
            groups += [lambda i=i, d=d: block(i) * (pltpu.roll(block(i), 8 - d, 0) if d else block(i))]
    groups += [lambda: jnp.ones((8, width), jnp.float32)]
    groups += [lambda: jnp.zeros((8, width), jnp.float32)] * 2
    return groups


def prepare_errors(se_ref, index_ref, se2_ref, rows_ref):
    for t in range(index_ref.shape[0]):
        rows_ref[t : t + 1, 0:R] = se_ref[pl.ds(index_ref[t], 1), :]
    squares = rows_ref[...] * rows_ref[...]
    for i in range(R):
        se2_ref[i] = jnp.broadcast_to(squares[:, i : i + 1], se2_ref.shape[1:])


def prepare(root_ref, grid_ref, base_ref, level_ref, covar_ref, cov_ref):
    units = root_ref.shape[1]
    span = 128 // units
    comps = base_ref.shape[1]
    cov_ref[R * units :, :] = jnp.zeros((cov_ref.shape[0] - R * units, 128), jnp.float32)
    for u in range(units):
        root = root_ref[:, u, :]
        cov_ref[pl.ds(u, R, stride=units), 0:R] = lax.dot_general(
            root, root, (((1,), (1,)), ((), ())), precision=HIGHEST, preferred_element_type=jnp.float32
        )
    line = lax.broadcasted_iota(jnp.int32, (128, comps), 0)
    scale = jnp.zeros((1, comps), jnp.float32)
    for n in range(grid_ref.shape[0]):
        scale = jnp.where(level_ref[...] == n, grid_ref[n], scale)
    scale2 = scale * scale
    pick = jnp.concatenate(
        [(line == base_ref[...] + n * units).astype(jnp.float32) for n in range(span)], axis=1
    ).astype(jnp.bfloat16)
    blocks = cov_ref.shape[0] // 128
    rest = jnp.concatenate([cov_ref[n * 128 : n * 128 + 128, :].T[0:56] for n in range(blocks)], axis=0)
    total = None
    for _ in range(3):
        head = rest.astype(jnp.bfloat16)
        term = jnp.dot(head, pick, preferred_element_type=jnp.float32)
        total = term if total is None else total + term
        rest = rest - head.astype(jnp.float32)
    for i in range(R):
        block, n = divmod(i, span)
        covar_ref[i] = total[block * 56 : block * 56 + 56, n * 128 : n * 128 + 128] * scale2


def sweep_kernel(
    se_in, index_in, root_in, grid_in, base_in, level_in, weight_in, e_in, w_ref, e_ref,
    se_ref, index_ref, root_ref, grid_ref, base_ref, level_ref, weight_ref, sems,
    covar_ref, se2_ref, cov_ref, rows_ref, d_ref, b_ref, c_ref, v_ref, x_ref,
):
    sources = (se_in, index_in, root_in, grid_in, base_in, level_in, weight_in)
    places = (se_ref, index_ref, root_ref, grid_ref, base_ref, level_ref, weight_ref)
    copies = [pltpu.make_async_copy(a, b, sems.at[n]) for n, (a, b) in enumerate(zip(sources, places))]
    for copy in copies:
        copy.start()
    for n in (0, 1, 3, 4, 5, 6):
        copies[n].wait()
    prepare_errors(se_ref, index_ref, se2_ref, rows_ref)
    copies[2].wait()
    effects = pltpu.make_async_copy(e_in, e_ref, sems.at[len(copies)])
    effects.start()
    prepare(root_ref, grid_ref, base_ref, level_ref, covar_ref, cov_ref)
    invert_all(covar_ref, se2_ref, weight_ref, w_ref, d_ref, b_ref, c_ref, v_ref, x_ref)
    effects.wait()


def sweep_stage(effects, se_table, se_index, base_root, grid_scale, comp_base, comp_grid, weights):
    tissues = se_table.shape[1]
    units = base_root.shape[0]
    tiles = se_index.shape[0]
    comps = comp_base.shape[0]
    panel = pltpu.VMEM((2 * NBLK * 64 * 8, 128), jnp.float32)
    operands = (
        se_table, se_index, base_root.transpose(1, 0, 2), grid_scale,
        comp_base.reshape(1, comps), comp_grid.reshape(1, comps), weights.reshape(1, comps), effects,
    )
    return pl.pallas_call(
        sweep_kernel,
        in_specs=[pl.BlockSpec(memory_space=pltpu.HBM)] * 8,
        out_specs=[pl.BlockSpec(memory_space=pltpu.VMEM)] * 2,
        out_shape=[pltpu.VMEM((2 * FEATS * 8, 128), jnp.float32), pltpu.VMEM(effects.shape, jnp.float32)],
        scratch_shapes=[
            pltpu.VMEM(se_table.shape, jnp.float32),
            pltpu.SMEM((tiles,), jnp.int32),
            pltpu.VMEM((tissues, units, tissues), jnp.float32),
            pltpu.SMEM(grid_scale.shape, jnp.float32),
            pltpu.VMEM((1, comps), jnp.int32),
            pltpu.VMEM((1, comps), jnp.int32),
            pltpu.VMEM((1, comps), jnp.float32),
            pltpu.SemaphoreType.DMA((8,)),
            pltpu.VMEM((R, 56, comps), jnp.float32),
            pltpu.VMEM((R, tiles, comps), jnp.float32),
            pltpu.VMEM((-(-R * units // 128) * 128, 128), jnp.float32),
            pltpu.VMEM((tiles, 128), jnp.float32),
            panel,
            panel,
            panel,
            pltpu.VMEM((2 * 64 * 8, 128), jnp.float32),
            pltpu.VMEM((2 * 72 * 8, 128), jnp.float32),
        ],
        compiler_params=pltpu.CompilerParams(vmem_limit_bytes=32 * 1024 * 1024),
        cost_estimate=pl.CostEstimate(flops=250_000_000, bytes_accessed=60_000_000, transcendentals=0),
        name="sweep",
    )(*(pltpu.with_memory_space_constraint(operand, pltpu.HBM) for operand in operands))


def build_chunk(t, chunk, e_ref, w_ref, hi_ref, lo_ref, left_ref):
    first = (t // 8) * (FEATS * 8) + t % 8
    for n in (2 * chunk, 2 * chunk + 1):
        part = w_ref[pl.ds(first + n * 1024, 128, stride=8), :].T
        head = part.astype(jnp.bfloat16)
        left_ref[0:128, n * 128 : (n + 1) * 128] = head
        left_ref[128:256, n * 128 : (n + 1) * 128] = (part - head.astype(jnp.float32)).astype(jnp.bfloat16)
    groups = product_groups(e_ref.at[:, pl.ds(pl.multiple_of(t * TILE, TILE), TILE)])
    for n in range(chunk * 32, chunk * 32 + 32, 2):
        both = jnp.concatenate([groups[n](), groups[n + 1]()], axis=0)
        head = both.astype(jnp.bfloat16)
        rest = (both - head.astype(jnp.float32)).astype(jnp.bfloat16)
        hi_ref[n * 8 : n * 8 + 16, :] = head
        lo_ref[n * 8 : n * 8 + 16, :] = rest


def score_and_build(t, now, later, following, e_ref, w_ref, scores_ref, stats_ref):
    hi_ref, lo_ref, left_ref = now
    scores = None
    for chunk in range(FEATS // 256):
        rows = slice(chunk * 256, chunk * 256 + 256)
        main = jnp.dot(left_ref[:, rows], hi_ref[rows, :], preferred_element_type=jnp.float32)
        rest = jnp.dot(left_ref[0:128, rows], lo_ref[rows, :], preferred_element_type=jnp.float32)
        part = main[0:128] + (main[128:256] + rest)
        scores = part if scores is None else scores + part
        build_chunk(later, chunk, e_ref, w_ref, *following)
    cols = pl.ds(pl.multiple_of(t * TILE, TILE), TILE)
    top = jnp.max(scores, axis=0, keepdims=True)
    scores_ref[:, cols] = scores
    stats_ref[0:1, cols] = top
    stats_ref[1:2, cols] = jnp.sum(jnp.exp(scores - top), axis=0, keepdims=True)


def tile_kernel(
    count, all_pairs, all_comps, e_ref, w_ref, resp_ref, loglik_ref, logw_ref,
    hi_a, lo_a, left_a, hi_b, lo_b, left_b, scores_ref, stats_ref,
    other_ref, mine_ref, slots_ref, pair_sems, mass_sems,
):
    chip, core = lax.axis_index("pairs"), lax.axis_index("comp")
    mesh_id = pl.DeviceIdType.MESH
    barrier = pltpu.get_barrier_semaphore()
    pl.semaphore_signal(barrier, inc=1, device_id=(chip, 1 - core), device_id_type=mesh_id)

    def greet(peer, _):
        pl.semaphore_signal(barrier, inc=1, device_id=(peer, core), device_id_type=mesh_id)
        return 0

    lax.fori_loop(0, chip, greet, 0)
    lax.fori_loop(chip + 1, count, greet, 0)
    tiles = e_ref.shape[1] // TILE
    one, two = (hi_a, lo_a, left_a), (hi_b, lo_b, left_b)
    for chunk in range(FEATS // 256):
        build_chunk(0, chunk, e_ref, w_ref, *one)

    def two_tiles(s, _):
        score_and_build(2 * s, one, 2 * s + 1, two, e_ref, w_ref, scores_ref, stats_ref)
        score_and_build(2 * s + 1, two, (2 * s + 2) % tiles, one, e_ref, w_ref, scores_ref, stats_ref)
        return 0

    width = e_ref.shape[1] // 2

    def swap(h):
        cols = pl.ds(pl.multiple_of(h * width, width), width)
        return pltpu.make_async_remote_copy(
            src_ref=stats_ref.at[:, cols], dst_ref=other_ref.at[:, cols],
            send_sem=pair_sems.at[0, h], recv_sem=pair_sems.at[1, h],
            device_id=(chip, 1 - core), device_id_type=mesh_id,
        )

    def half(h, _):
        lax.fori_loop(0, tiles // 4, lambda s, z: two_tiles(h * (tiles // 4) + s, z), 0)

        @pl.when(h == 0)
        def _():
            pl.semaphore_wait(barrier, count)

        swap(h).start()
        return 0

    lax.fori_loop(0, 2, half, 0)

    def one_part(n, mass):
        cols = pl.ds(pl.multiple_of(n * TILE, TILE), TILE)
        m0, m1 = stats_ref[0:1, cols], other_ref[0:1, cols]
        top = jnp.maximum(m0, m1)
        total = stats_ref[1:2, cols] * jnp.exp(m0 - top) + other_ref[1:2, cols] * jnp.exp(m1 - top)
        loglik = top + jnp.log(total)
        loglik_ref[0:1, cols] = loglik
        resp = jnp.exp(scores_ref[:, cols] - loglik)
        resp_ref[:, cols] = resp
        for j in range(TILE // 128):
            mass = mass + resp[:, j * 128 : (j + 1) * 128]
        return mass

    def two_parts(n, mass):
        return one_part(2 * n + 1, one_part(2 * n, mass))

    def half_parts(h, mass):
        swap(h).wait()
        return lax.fori_loop(h * (tiles // 4), (h + 1) * (tiles // 4), two_parts, mass)

    mass = lax.fori_loop(0, 2, half_parts, jnp.zeros((128, 128), jnp.float32))
    own = jnp.sum(mass.T, axis=0, keepdims=True)
    mine_ref[...] = own
    slots_ref[chip] = own

    def send(n, _):
        far = 1 + (n + (2 * count) // 3 - 1) % (count - 1)
        pltpu.make_async_remote_copy(
            src_ref=mine_ref, dst_ref=slots_ref.at[chip], send_sem=mass_sems.at[0], recv_sem=mass_sems.at[1],
            device_id=((chip + far) % count, core), device_id_type=mesh_id,
        ).start()
        return 0

    lax.fori_loop(0, count - 1, send, 0)
    every = pltpu.make_async_remote_copy(
        src_ref=slots_ref.at[pl.ds(0, count - 1)], dst_ref=slots_ref.at[pl.ds(0, count - 1)],
        send_sem=mass_sems.at[0], recv_sem=mass_sems.at[1],
        device_id=((chip + 1) % count, core), device_id_type=mesh_id,
    )
    every.wait_recv()
    parts = [slots_ref[n] for n in range(count)]
    while len(parts) > 1:
        parts = [parts[n] + parts[n + 1] for n in range(0, len(parts), 2)]
    logw_ref[...] = jnp.log((parts[0] + 1.0) / (all_pairs + all_comps))
    every.wait_send()


def write_kernel(resp_ref, loglik_ref, logw_ref, resp_out, loglik_out, logw_out, sems):
    pairs = ((resp_ref, resp_out), (loglik_ref, loglik_out), (logw_ref, logw_out))
    copies = [pltpu.make_async_copy(a, b, sems.at[n]) for n, (a, b) in enumerate(pairs)]
    for copy in copies:
        copy.start()
    for copy in copies:
        copy.wait()


def per_device(effects, se_table, se_index, base_root, grid_scale, comp_base, comp_grid, weights):
    pairs = effects.shape[1]
    comps = comp_base.shape[0]
    w, near_effects = sweep_stage(
        effects, se_table, se_index, base_root, grid_scale, comp_base, comp_grid, weights
    )
    count = lax.axis_size("pairs")
    vmem = pl.BlockSpec(memory_space=pltpu.VMEM)
    products = [
        pltpu.VMEM((FEATS, TILE), jnp.bfloat16),
        pltpu.VMEM((FEATS, TILE), jnp.bfloat16),
        pltpu.VMEM((256, FEATS), jnp.bfloat16),
    ]
    shapes = ((comps, pairs), (1, pairs), (1, comps))
    results = pl.pallas_call(
        functools.partial(tile_kernel, count, pairs * count, comps * lax.axis_size("comp")),
        in_specs=[vmem, vmem],
        out_specs=[vmem, vmem, vmem],
        out_shape=[pltpu.VMEM(shape, jnp.float32) for shape in shapes],
        scratch_shapes=products + products + [
            pltpu.VMEM((comps, pairs), jnp.float32),
            pltpu.VMEM((2, pairs), jnp.float32),
            pltpu.VMEM((2, pairs), jnp.float32),
            pltpu.VMEM((1, comps), jnp.float32),
            pltpu.VMEM((count, 1, comps), jnp.float32),
            pltpu.SemaphoreType.DMA((2, 2)),
            pltpu.SemaphoreType.DMA((2,)),
        ],
        compiler_params=pltpu.CompilerParams(
            collective_id=0, has_side_effects=True, vmem_limit_bytes=24 * 1024 * 1024,
        ),
        name="tiles",
    )(near_effects, w)
    resp, loglik, logw = pl.pallas_call(
        write_kernel,
        in_specs=[vmem, vmem, vmem],
        out_specs=[pl.BlockSpec(memory_space=pltpu.HBM)] * 3,
        out_shape=[jax.ShapeDtypeStruct(shape, jnp.float32) for shape in shapes],
        scratch_shapes=[pltpu.SemaphoreType.DMA((3,))],
        compiler_params=pltpu.CompilerParams(vmem_limit_bytes=4 * 1024 * 1024),
        name="write",
    )(*results)
    return (resp, logw.reshape(comps), loglik.reshape(pairs))


def solution(mesh):
    placed = (P(None, "pairs"), P(), P("pairs"), P(), P(), P("comp"), P("comp"), P("comp"))
    return jax.shard_map(
        per_device,
        mesh=mesh,
        in_specs=placed,
        out_specs=(P("comp", "pairs"), P("comp"), P("pairs")),
        check_vma=False,
    )
```

```python
import functools
import math

import jax
import jax.numpy as jnp
from jax import lax
from jax.experimental import pallas as pl
from jax.experimental.pallas import tpu as pltpu
from jax.sharding import PartitionSpec as P

TILE = 512
R = 49
NBLK = 6
FEATS = 1280
OFF_BORDER = 960
OFF_LAST = 1008
OFF_DIAG = 1016
OFF_BIAS = 1256
HIGHEST = lax.Precision.HIGHEST


def row8(index):
    return pl.ds(pl.multiple_of(index * 8, 8), 8)


def invert_all(covar_ref, se2_ref, weight_ref, w_ref, d_ref, b_ref, c_ref, v_ref, x_ref):
    def w_at(g, f):
        return row8(g * FEATS + f)

    def d_at(g, block, a, c):
        return row8((g * NBLK + block) * 64 + a * 8 + c)

    def p_at(g, block, a, c):
        return row8((g * NBLK + block) * 64 + a * 8 + c)

    def pair_base(i, j):
        return (i * (i - 1) // 2 + j) * 64

    def cov(i, j):
        return jnp.broadcast_to(covar_ref[i, pl.ds(j, 1), :], (8, 128))

    def x_at(g, n):
        return row8(g * 72 + n)

    for g in range(2):
        se_last = se2_ref[48, g * 8 : g * 8 + 8, :]
        pivot = cov(48, 48) + se_last
        inv = 1.0 / pivot
        x_ref[x_at(g, 48), :] = jnp.log(pivot)
        w_ref[w_at(g, OFF_LAST), :] = -inv
        for i in range(48):
            edge = cov(48, i)
            x_ref[x_at(g, i), :] = edge
            w_ref[w_at(g, OFF_BORDER + i), :] = edge * inv

    def init_row(i, _):
        edges = {(g, a): x_ref[x_at(g, i * 8 + a), :] for g in range(2) for a in range(8)}

        def init_pair(j, _):
            scaled = {(g, c): w_ref[w_at(g, OFF_BORDER + j * 8 + c), :] for g in range(2) for c in range(8)}
            base = pair_base(i, j)
            for a in range(8):
                for c in range(8):
                    entry = cov(i * 8 + a, j * 8 + c)
                    for g in range(2):
                        w_ref[w_at(g, base + a * 8 + c), :] = entry - edges[g, a] * scaled[g, c]
            return 0

        lax.fori_loop(0, i, init_pair, 0)
        scaled = {(g, c): w_ref[w_at(g, OFF_BORDER + i * 8 + c), :] for g in range(2) for c in range(8)}
        for a in range(8):
            for c in range(a + 1):
                for g in range(2):
                    entry = cov(i * 8 + a, i * 8 + c) - edges[g, a] * scaled[g, c]
                    if a == c:
                        entry = entry + se2_ref[i * 8 + a, g * 8 : g * 8 + 8, :]
                    d_ref[d_at(g, i, a, c), :] = entry
        return 0

    lax.fori_loop(0, NBLK, init_row, 0)

    def pivot_block(k):
        for g in range(2):
            m = {(a, c): d_ref[d_at(g, k, a, c), :] for a in range(8) for c in range(a + 1)}
            product = None
            for s in range(8):
                p = m[s, s]
                product = p if product is None else product * p
                inv = 1.0 / p
                col = {a: (m[a, s] if a > s else m[s, a]) for a in range(8) if a != s}
                scaled = {a: col[a] * inv for a in col}
                for a in col:
                    for c in col:
                        if c <= a:
                            m[a, c] = m[a, c] - scaled[a] * col[c]
                for a in col:
                    m[max(a, s), min(a, s)] = scaled[a]
                m[s, s] = -inv
            x_ref[x_at(g, 48), :] = x_ref[x_at(g, 48), :] + jnp.log(product)
            for a in range(8):
                for c in range(8):
                    entry = m[max(a, c), min(a, c)]
                    if c <= a:
                        d_ref[d_at(g, k, a, c), :] = entry
                    v_ref[row8(g * 64 + a * 8 + c), :] = -entry

    def scale_block(g, k, j, swap):
        base = pair_base(k, j) if swap else pair_base(j, k)
        for half in range(4):
            rows = range(half // 2 * 4, half // 2 * 4 + 4)
            cols = range(half % 2 * 4, half % 2 * 4 + 4)
            acc = {}
            for l in range(8):
                left = {}
                for a in rows:
                    if half % 2:
                        left[a] = c_ref[p_at(g, j, a, l), :]
                    else:
                        left[a] = w_ref[w_at(g, base + (l * 8 + a if swap else a * 8 + l)), :]
                        c_ref[p_at(g, j, a, l), :] = left[a]
                for c in cols:
                    right = v_ref[row8(g * 64 + l * 8 + c), :]
                    for a in rows:
                        term = left[a] * right
                        acc[a, c] = term if l == 0 else acc[a, c] + term
            for a in rows:
                for c in cols:
                    b_ref[p_at(g, j, a, c), :] = acc[a, c]
        for a in range(8):
            for c in range(8):
                w_ref[w_at(g, base + (c * 8 + a if swap else a * 8 + c)), :] = b_ref[p_at(g, j, a, c), :]

    def scale_border(g, k):
        old = [w_ref[w_at(g, OFF_BORDER + k * 8 + m), :] for m in range(8)]
        total = w_ref[w_at(g, OFF_LAST), :]
        for c in range(8):
            new = old[0] * v_ref[row8(g * 64 + c), :]
            for l in range(1, 8):
                new = new + old[l] * v_ref[row8(g * 64 + l * 8 + c), :]
            x_ref[x_at(g, 49 + c), :] = new
            w_ref[w_at(g, OFF_BORDER + k * 8 + c), :] = new
            total = total - new * old[c]
        w_ref[w_at(g, OFF_LAST), :] = total

    def update_pair(g, i, j):
        base = pair_base(i, j)
        for half in range(4):
            rows = range(half // 2 * 4, half // 2 * 4 + 4)
            cols = range(half % 2 * 4, half % 2 * 4 + 4)
            acc = {(a, c): w_ref[w_at(g, base + a * 8 + c), :] for a in rows for c in cols}
            for m in range(8):
                left = {a: b_ref[p_at(g, i, a, m), :] for a in rows}
                for c in cols:
                    right = c_ref[p_at(g, j, c, m), :]
                    for a in rows:
                        acc[a, c] = acc[a, c] - left[a] * right
            for a in rows:
                for c in cols:
                    w_ref[w_at(g, base + a * 8 + c), :] = acc[a, c]

    def update_diag(g, i):
        for rows in (range(0, 6), range(6, 8)):
            acc = {(a, c): d_ref[d_at(g, i, a, c), :] for a in rows for c in range(a + 1)}
            if rows[0]:
                edge = [w_ref[w_at(g, OFF_BORDER + i * 8 + c), :] for c in range(8)]
            for m in range(8):
                left = {a: b_ref[p_at(g, i, a, m), :] for a in rows}
                if rows[0]:
                    last = x_ref[x_at(g, 49 + m), :]
                for c in range(rows[-1] + 1):
                    right = c_ref[p_at(g, i, c, m), :]
                    for a in rows:
                        if c <= a:
                            acc[a, c] = acc[a, c] - left[a] * right
                    if rows[0]:
                        edge[c] = edge[c] - last * right
            for a, c in acc:
                d_ref[d_at(g, i, a, c), :] = acc[a, c]
            if rows[0]:
                for c in range(8):
                    w_ref[w_at(g, OFF_BORDER + i * 8 + c), :] = edge[c]

    def sweep(k, _):
        pivot_block(k)

        def scale_one(j, swap):
            for g in range(2):
                scale_block(g, k, j, swap)

        lax.fori_loop(0, k, lambda j, z: (scale_one(j, True), z)[1], 0)
        lax.fori_loop(k + 1, NBLK, lambda j, z: (scale_one(j, False), z)[1], 0)
        for g in range(2):
            scale_border(g, k)

        def update_row(t, _):
            i = t + (t >= k).astype(jnp.int32)

            def update_one(s, _):
                for g in range(2):
                    update_pair(g, i, s + (s >= k).astype(jnp.int32))
                return 0

            lax.fori_loop(0, t, update_one, 0)
            for g in range(2):
                update_diag(g, i)
            return 0

        lax.fori_loop(0, NBLK - 1, update_row, 0)
        return 0

    lax.fori_loop(0, NBLK, sweep, 0)

    zero = jnp.zeros((8, 128), jnp.float32)
    constant = 0.5 * R * math.log(2.0 * math.pi)

    def finish(g, _):
        w_ref[w_at(g, OFF_LAST), :] = 0.5 * w_ref[w_at(g, OFF_LAST), :]
        for n in range(1, 8):
            w_ref[w_at(g, OFF_LAST + n), :] = zero

        def finish_diag(i, _):
            for d in range(5):
                weight = 1.0 if 0 < d < 4 else 0.5
                for c in range(8):
                    a = (c + d) % 8
                    entry = d_ref[d_at(g, i, max(a, c), min(a, c)), :]
                    w_ref[w_at(g, OFF_DIAG + i * 40 + d * 8 + c), :] = weight * entry
            return 0

        lax.fori_loop(0, NBLK, finish_diag, 0)
        bias = jnp.broadcast_to(jnp.log(weight_ref[...]), (8, 128)) - 0.5 * x_ref[x_at(g, 48), :] - constant
        coarse = bias.astype(jnp.bfloat16).astype(jnp.float32)
        w_ref[w_at(g, OFF_BIAS), :] = coarse
        w_ref[w_at(g, OFF_BIAS + 1), :] = bias - coarse
        for n in range(OFF_BIAS + 2, FEATS):
            w_ref[w_at(g, n), :] = zero
        return 0

    lax.fori_loop(0, 2, finish, 0)


def product_groups(e_ref):
    width = e_ref.shape[1]

    def block(i):
        return e_ref[i * 8 : i * 8 + 8, :]

    def row(i):
        return jnp.broadcast_to(e_ref[i : i + 1, :], (8, width))

    groups = []
    for i in range(NBLK):
        for j in range(i):
            groups += [lambda i=i, j=j, a=a: row(i * 8 + a) * block(j) for a in range(8)]
    groups += [lambda j=j: row(48) * block(j) for j in range(NBLK)]
    groups += [lambda: row(48) * row(48)]
    for i in range(NBLK):
        for d in range(5):
            groups += [lambda i=i, d=d: block(i) * (pltpu.roll(block(i), 8 - d, 0) if d else block(i))]
    groups += [lambda: jnp.ones((8, width), jnp.float32)]
    groups += [lambda: jnp.zeros((8, width), jnp.float32)] * 2
    return groups


def prepare_errors(se_ref, index_ref, se2_ref, rows_ref):
    for t in range(index_ref.shape[0]):
        rows_ref[t : t + 1, 0:R] = se_ref[pl.ds(index_ref[t], 1), :]
    squares = rows_ref[...] * rows_ref[...]
    for i in range(R):
        se2_ref[i] = jnp.broadcast_to(squares[:, i : i + 1], se2_ref.shape[1:])


def prepare(root_ref, grid_ref, base_ref, level_ref, covar_ref, cov_ref):
    units = root_ref.shape[1]
    span = 128 // units
    comps = base_ref.shape[1]
    cov_ref[R * units :, :] = jnp.zeros((cov_ref.shape[0] - R * units, 128), jnp.float32)
    for u in range(units):
        root = root_ref[:, u, :]
        cov_ref[pl.ds(u, R, stride=units), 0:R] = lax.dot_general(
            root, root, (((1,), (1,)), ((), ())), precision=HIGHEST, preferred_element_type=jnp.float32
        )
    line = lax.broadcasted_iota(jnp.int32, (128, comps), 0)
    scale = jnp.zeros((1, comps), jnp.float32)
    for n in range(grid_ref.shape[0]):
        scale = jnp.where(level_ref[...] == n, grid_ref[n], scale)
    scale2 = scale * scale
    pick = jnp.concatenate(
        [(line == base_ref[...] + n * units).astype(jnp.float32) for n in range(span)], axis=1
    ).astype(jnp.bfloat16)
    blocks = cov_ref.shape[0] // 128
    rest = jnp.concatenate([cov_ref[n * 128 : n * 128 + 128, :].T[0:56] for n in range(blocks)], axis=0)
    total = None
    for _ in range(3):
        head = rest.astype(jnp.bfloat16)
        term = jnp.dot(head, pick, preferred_element_type=jnp.float32)
        total = term if total is None else total + term
        rest = rest - head.astype(jnp.float32)
    for i in range(R):
        block, n = divmod(i, span)
        covar_ref[i] = total[block * 56 : block * 56 + 56, n * 128 : n * 128 + 128] * scale2


def sweep_kernel(
    se_in, index_in, root_in, grid_in, base_in, level_in, weight_in, e_in, w_ref, e_ref,
    se_ref, index_ref, root_ref, grid_ref, base_ref, level_ref, weight_ref, sems,
    covar_ref, se2_ref, cov_ref, rows_ref, d_ref, b_ref, c_ref, v_ref, x_ref,
):
    sources = (se_in, index_in, root_in, grid_in, base_in, level_in, weight_in)
    places = (se_ref, index_ref, root_ref, grid_ref, base_ref, level_ref, weight_ref)
    copies = [pltpu.make_async_copy(a, b, sems.at[n]) for n, (a, b) in enumerate(zip(sources, places))]
    for copy in copies:
        copy.start()
    for n in (0, 1, 3, 4, 5, 6):
        copies[n].wait()
    prepare_errors(se_ref, index_ref, se2_ref, rows_ref)
    copies[2].wait()
    effects = pltpu.make_async_copy(e_in, e_ref, sems.at[len(copies)])
    effects.start()
    prepare(root_ref, grid_ref, base_ref, level_ref, covar_ref, cov_ref)
    invert_all(covar_ref, se2_ref, weight_ref, w_ref, d_ref, b_ref, c_ref, v_ref, x_ref)
    effects.wait()


def sweep_stage(effects, se_table, se_index, base_root, grid_scale, comp_base, comp_grid, weights):
    tissues = se_table.shape[1]
    units = base_root.shape[0]
    tiles = se_index.shape[0]
    comps = comp_base.shape[0]
    panel = pltpu.VMEM((2 * NBLK * 64 * 8, 128), jnp.float32)
    operands = (
        se_table, se_index, base_root.transpose(1, 0, 2), grid_scale,
        comp_base.reshape(1, comps), comp_grid.reshape(1, comps), weights.reshape(1, comps), effects,
    )
    return pl.pallas_call(
        sweep_kernel,
        in_specs=[pl.BlockSpec(memory_space=pltpu.HBM)] * 8,
        out_specs=[pl.BlockSpec(memory_space=pltpu.VMEM)] * 2,
        out_shape=[pltpu.VMEM((2 * FEATS * 8, 128), jnp.float32), pltpu.VMEM(effects.shape, jnp.float32)],
        scratch_shapes=[
            pltpu.VMEM(se_table.shape, jnp.float32),
            pltpu.SMEM((tiles,), jnp.int32),
            pltpu.VMEM((tissues, units, tissues), jnp.float32),
            pltpu.SMEM(grid_scale.shape, jnp.float32),
            pltpu.VMEM((1, comps), jnp.int32),
            pltpu.VMEM((1, comps), jnp.int32),
            pltpu.VMEM((1, comps), jnp.float32),
            pltpu.SemaphoreType.DMA((8,)),
            pltpu.VMEM((R, 56, comps), jnp.float32),
            pltpu.VMEM((R, tiles, comps), jnp.float32),
            pltpu.VMEM((-(-R * units // 128) * 128, 128), jnp.float32),
            pltpu.VMEM((tiles, 128), jnp.float32),
            panel,
            panel,
            panel,
            pltpu.VMEM((2 * 64 * 8, 128), jnp.float32),
            pltpu.VMEM((2 * 72 * 8, 128), jnp.float32),
        ],
        compiler_params=pltpu.CompilerParams(vmem_limit_bytes=32 * 1024 * 1024),
        cost_estimate=pl.CostEstimate(flops=250_000_000, bytes_accessed=60_000_000, transcendentals=0),
        name="sweep",
    )(*(pltpu.with_memory_space_constraint(operand, pltpu.HBM) for operand in operands))


def build_chunk(t, chunk, e_ref, w_ref, hi_ref, lo_ref, left_ref):
    first = (t // 8) * (FEATS * 8) + t % 8
    for n in (2 * chunk, 2 * chunk + 1):
        part = w_ref[pl.ds(first + n * 1024, 128, stride=8), :].T
        head = part.astype(jnp.bfloat16)
        left_ref[0:128, n * 128 : (n + 1) * 128] = head
        left_ref[128:256, n * 128 : (n + 1) * 128] = (part - head.astype(jnp.float32)).astype(jnp.bfloat16)
    groups = product_groups(e_ref.at[:, pl.ds(pl.multiple_of(t * TILE, TILE), TILE)])
    for n in range(chunk * 32, chunk * 32 + 32, 2):
        both = jnp.concatenate([groups[n](), groups[n + 1]()], axis=0)
        head = both.astype(jnp.bfloat16)
        rest = (both - head.astype(jnp.float32)).astype(jnp.bfloat16)
        hi_ref[n * 8 : n * 8 + 16, :] = head
        lo_ref[n * 8 : n * 8 + 16, :] = rest


def score_and_build(t, now, later, following, e_ref, w_ref, scores_ref, stats_ref):
    hi_ref, lo_ref, left_ref = now
    scores = None
    for chunk in range(FEATS // 256):
        rows = slice(chunk * 256, chunk * 256 + 256)
        main = jnp.dot(left_ref[:, rows], hi_ref[rows, :], preferred_element_type=jnp.float32)
        rest = jnp.dot(left_ref[0:128, rows], lo_ref[rows, :], preferred_element_type=jnp.float32)
        part = main[0:128] + (main[128:256] + rest)
        scores = part if scores is None else scores + part
        build_chunk(later, chunk, e_ref, w_ref, *following)
    cols = pl.ds(pl.multiple_of(t * TILE, TILE), TILE)
    top = jnp.max(scores, axis=0, keepdims=True)
    scores_ref[:, cols] = scores
    stats_ref[0:1, cols] = top
    stats_ref[1:2, cols] = jnp.sum(jnp.exp(scores - top), axis=0, keepdims=True)


def tile_kernel(
    count, all_pairs, all_comps, e_ref, w_ref, resp_ref, loglik_ref, logw_ref,
    hi_a, lo_a, left_a, hi_b, lo_b, left_b, scores_ref, stats_ref,
    other_ref, mine_ref, slots_ref, pair_sems, mass_sems,
):
    chip, core = lax.axis_index("pairs"), lax.axis_index("comp")
    mesh_id = pl.DeviceIdType.MESH
    barrier = pltpu.get_barrier_semaphore()
    pl.semaphore_signal(barrier, inc=1, device_id=(chip, 1 - core), device_id_type=mesh_id)

    def greet(peer, _):
        pl.semaphore_signal(barrier, inc=1, device_id=(peer, core), device_id_type=mesh_id)
        return 0

    lax.fori_loop(0, chip, greet, 0)
    lax.fori_loop(chip + 1, count, greet, 0)
    tiles = e_ref.shape[1] // TILE
    one, two = (hi_a, lo_a, left_a), (hi_b, lo_b, left_b)
    for chunk in range(FEATS // 256):
        build_chunk(0, chunk, e_ref, w_ref, *one)

    def two_tiles(s, _):
        score_and_build(2 * s, one, 2 * s + 1, two, e_ref, w_ref, scores_ref, stats_ref)
        score_and_build(2 * s + 1, two, (2 * s + 2) % tiles, one, e_ref, w_ref, scores_ref, stats_ref)
        return 0

    width = e_ref.shape[1] // 2

    def swap(h):
        cols = pl.ds(pl.multiple_of(h * width, width), width)
        return pltpu.make_async_remote_copy(
            src_ref=stats_ref.at[:, cols], dst_ref=other_ref.at[:, cols],
            send_sem=pair_sems.at[0, h], recv_sem=pair_sems.at[1, h],
            device_id=(chip, 1 - core), device_id_type=mesh_id,
        )

    def half(h, _):
        lax.fori_loop(0, tiles // 4, lambda s, z: two_tiles(h * (tiles // 4) + s, z), 0)

        @pl.when(h == 0)
        def _():
            pl.semaphore_wait(barrier, count)

        swap(h).start()
        return 0

    lax.fori_loop(0, 2, half, 0)

    def one_part(n, mass):
        cols = pl.ds(pl.multiple_of(n * TILE, TILE), TILE)
        m0, m1 = stats_ref[0:1, cols], other_ref[0:1, cols]
        top = jnp.maximum(m0, m1)
        total = stats_ref[1:2, cols] * jnp.exp(m0 - top) + other_ref[1:2, cols] * jnp.exp(m1 - top)
        loglik = top + jnp.log(total)
        loglik_ref[0:1, cols] = loglik
        resp = jnp.exp(scores_ref[:, cols] - loglik)
        resp_ref[:, cols] = resp
        for j in range(TILE // 128):
            mass = mass + resp[:, j * 128 : (j + 1) * 128]
        return mass

    def two_parts(n, mass):
        return one_part(2 * n + 1, one_part(2 * n, mass))

    def half_parts(h, mass):
        swap(h).wait()
        return lax.fori_loop(h * (tiles // 4), (h + 1) * (tiles // 4), two_parts, mass)

    mass = lax.fori_loop(0, 2, half_parts, jnp.zeros((128, 128), jnp.float32))
    own = jnp.sum(mass.T, axis=0, keepdims=True)
    mine_ref[...] = own
    slots_ref[chip] = own

    def send(peer, _):
        pltpu.make_async_remote_copy(
            src_ref=mine_ref, dst_ref=slots_ref.at[chip], send_sem=mass_sems.at[0], recv_sem=mass_sems.at[1],
            device_id=(peer, core), device_id_type=mesh_id,
        ).start()
        return 0

    lax.fori_loop(chip + 1, count, send, 0)
    lax.fori_loop(0, chip, send, 0)
    every = pltpu.make_async_remote_copy(
        src_ref=slots_ref.at[pl.ds(0, count - 1)], dst_ref=slots_ref.at[pl.ds(0, count - 1)],
        send_sem=mass_sems.at[0], recv_sem=mass_sems.at[1],
        device_id=((chip + 1) % count, core), device_id_type=mesh_id,
    )
    every.wait_recv()
    parts = [slots_ref[n] for n in range(count)]
    while len(parts) > 1:
        parts = [parts[n] + parts[n + 1] for n in range(0, len(parts), 2)]
    logw_ref[...] = jnp.log((parts[0] + 1.0) / (all_pairs + all_comps))
    every.wait_send()


def write_kernel(resp_ref, loglik_ref, logw_ref, resp_out, loglik_out, logw_out, sems):
    pairs = ((resp_ref, resp_out), (loglik_ref, loglik_out), (logw_ref, logw_out))
    copies = [pltpu.make_async_copy(a, b, sems.at[n]) for n, (a, b) in enumerate(pairs)]
    for copy in copies:
        copy.start()
    for copy in copies:
        copy.wait()


def per_device(effects, se_table, se_index, base_root, grid_scale, comp_base, comp_grid, weights):
    pairs = effects.shape[1]
    comps = comp_base.shape[0]
    w, near_effects = sweep_stage(
        effects, se_table, se_index, base_root, grid_scale, comp_base, comp_grid, weights
    )
    count = lax.axis_size("pairs")
    vmem = pl.BlockSpec(memory_space=pltpu.VMEM)
    products = [
        pltpu.VMEM((FEATS, TILE), jnp.bfloat16),
        pltpu.VMEM((FEATS, TILE), jnp.bfloat16),
        pltpu.VMEM((256, FEATS), jnp.bfloat16),
    ]
    shapes = ((comps, pairs), (1, pairs), (1, comps))
    results = pl.pallas_call(
        functools.partial(tile_kernel, count, pairs * count, comps * lax.axis_size("comp")),
        in_specs=[vmem, vmem],
        out_specs=[vmem, vmem, vmem],
        out_shape=[pltpu.VMEM(shape, jnp.float32) for shape in shapes],
        scratch_shapes=products + products + [
            pltpu.VMEM((comps, pairs), jnp.float32),
            pltpu.VMEM((2, pairs), jnp.float32),
            pltpu.VMEM((2, pairs), jnp.float32),
            pltpu.VMEM((1, comps), jnp.float32),
            pltpu.VMEM((count, 1, comps), jnp.float32),
            pltpu.SemaphoreType.DMA((2, 2)),
            pltpu.SemaphoreType.DMA((2,)),
        ],
        compiler_params=pltpu.CompilerParams(
            collective_id=0, has_side_effects=True, vmem_limit_bytes=24 * 1024 * 1024,
        ),
        name="tiles",
    )(near_effects, w)
    resp, loglik, logw = pl.pallas_call(
        write_kernel,
        in_specs=[vmem, vmem, vmem],
        out_specs=[pl.BlockSpec(memory_space=pltpu.HBM)] * 3,
        out_shape=[jax.ShapeDtypeStruct(shape, jnp.float32) for shape in shapes],
        scratch_shapes=[pltpu.SemaphoreType.DMA((3,))],
        compiler_params=pltpu.CompilerParams(vmem_limit_bytes=4 * 1024 * 1024),
        name="write",
    )(*results)
    return (resp, logw.reshape(comps), loglik.reshape(pairs))


def solution(mesh):
    placed = (P(None, "pairs"), P(), P("pairs"), P(), P(), P("comp"), P("comp"), P("comp"))
    return jax.shard_map(
        per_device,
        mesh=mesh,
        in_specs=placed,
        out_specs=(P("comp", "pairs"), P("comp"), P("pairs")),
        check_vma=False,
    )
```
